32 devices in a mesh: row: 8 (over y, x, core), col: 4 (over z).
Axes of the slice: x: 2, y: 2, z: 4, core: 2. Of those that a mesh axis runs over, the one named last changes fastest.
Arguments:
- pair_state: bfloat16 [128, 128, 128], P('row', 'col'), may hold values from -6 to 6
- pair_mask: int32 [128, 128], P('row', 'col'), may hold values 0 or 1
- input_gain: float32 [2, 128], replicated, may hold values from 0.25 to 1.75
- input_bias: float32 [2, 128], replicated, may hold values from -1.5 to 1.5
- proj_weights: bfloat16 [2, 128, 512], replicated, may hold values from -0.5 to 0.5
- gate_weights: bfloat16 [2, 128, 128], replicated, may hold values from -0.5 to 0.5
- output_gain: float32 [2, 128], replicated, may hold values from 0.25 to 1.75
- output_bias: float32 [2, 128], replicated, may hold values from -1.5 to 1.5
- output_weights: bfloat16 [2, 128, 128], replicated, may hold values from -0.5 to 0.5
Outputs:
- pair_out: bfloat16 [128, 128, 128], P('row', 'col')
The draws below stay inside these ranges and needn't reach their ends.
All inputs are finite; a program needn't handle non-finite values. No bound on the sum of `pair_mask` on one device may be relied on, other than what follows from the above.
Results may differ from the reference program's by a relative error of at most 0.0058.
Values may be sent and summed in bfloat16 or wider, within the bound.
A program may use at most 64 MiB of HBM per device.

```python
import jax
import jax.numpy as jnp
from jax import lax

CZ = 128
CH = 128
NTOK = 128


def plant(result, stream_key, low, largest):
    longest = result.shape.index(max(result.shape))
    spots = []
    for shift in (0, 1):
        where = [jax.random.randint(jax.random.fold_in(stream_key, axis), (), 0, length) for axis, length in enumerate(result.shape)]
        where[longest] = (where[longest] + shift) % result.shape[longest]
        spots.append(tuple(where))
    return result.at[spots[0]].set(low).at[spots[1]].set(largest)


def shard_levels(own_key, dims, split, smallest, high):
    factor_of, own = 1.0, jax.random.fold_in(own_key, 6)
    for axis_at, parts in split:
        draws = jnp.exp(jax.random.uniform(jax.random.fold_in(own, axis_at), (parts,), jnp.float32, smallest / len(split), high / len(split)))
        factor_of = factor_of * jnp.repeat(draws, dims[axis_at] // parts).reshape([-1 if axis == axis_at else 1 for axis in range(len(dims))])
    return factor_of


def scatter_about(key, shape, scale, reach, split=(), held_as=jnp.bfloat16):
    drawn = scale * jax.random.normal(key, shape, jnp.float32)
    if split:
        drawn = drawn * shard_levels(key, shape, split, -0.22, 0.18)
    return jnp.clip(drawn, -reach, reach).astype(held_as)


def setup_inputs(seed: int = 0) -> dict:
    arg_keys = jax.random.split(jax.random.key(seed), 10)
    return {
        "pair_state": scatter_about(arg_keys[0], (NTOK, NTOK, CZ), 1.0, 6.0, ((0, 8), (1, 4))),
        "pair_mask": plant((jax.random.randint(arg_keys[1], (NTOK, NTOK), 0, 5) < 4).astype(jnp.int32), jax.random.fold_in(arg_keys[1], 1), 0, 1),
        "input_gain": jnp.clip(1.0 + 0.15 * jax.random.normal(arg_keys[2], (2, CZ), jnp.float32), 0.25, 1.75),
        "input_bias": scatter_about(arg_keys[3], (2, CZ), 0.3, 1.5, (), jnp.float32),
        "proj_weights": scatter_about(arg_keys[4], (2, CZ, 4 * CH), CZ ** -0.5, 0.5),
        "gate_weights": scatter_about(arg_keys[5], (2, CZ, CZ), CZ ** -0.5, 0.5),
        "output_gain": jnp.clip(1.0 + 0.15 * jax.random.normal(arg_keys[6], (2, CH), jnp.float32), 0.25, 1.75),
        "output_bias": scatter_about(arg_keys[7], (2, CH), 0.3, 1.5, (), jnp.float32),
        "output_weights": scatter_about(arg_keys[8], (2, CH, CZ), CH ** -0.5, 0.5),
    }


epsilon = 1e-05
group_width = 16

def normalize(values, weight_scale, weight_shift, reduce_axis):
    average = lax.optimization_barrier(jnp.mean(values, axis=reduce_axis, keepdims=True))
    centred = values - average
    spread = lax.optimization_barrier(jnp.mean(centred * centred, axis=reduce_axis, keepdims=True))
    return centred * lax.rsqrt(spread + epsilon) * weight_scale + weight_shift

def triangle(current, mask_float, layer_index, input_gain, input_bias, proj_weights, gate_weights, output_gain, output_bias, output_weights):
    pair_ln = normalize(current, input_gain[layer_index], input_bias[layer_index], -1).astype(jnp.bfloat16)
    flattened = pair_ln.reshape(NTOK * NTOK, CZ)
    gate_value = jax.nn.sigmoid(jnp.dot(flattened, gate_weights[layer_index], preferred_element_type=jnp.float32)).reshape(NTOK, NTOK, CZ)
    weights = proj_weights[layer_index]

    def channel_group(group_index):
        first_col = (group_index * group_width).astype(jnp.int32)
        pieces = []
        for offset in range(4):
            columns = lax.dynamic_slice_in_dim(weights, first_col + offset * CH, group_width, 1)
            pieces.append(jnp.dot(flattened, columns, preferred_element_type=jnp.float32).reshape(NTOK, NTOK, group_width))
        left_panel = (jax.nn.sigmoid(pieces[0]) * pieces[1] * mask_float).astype(jnp.bfloat16)
        right_panel = (jax.nn.sigmoid(pieces[2]) * pieces[3] * mask_float).astype(jnp.bfloat16)
        left_panel = lax.optimization_barrier(left_panel).astype(jnp.float32)
        right_panel = lax.optimization_barrier(right_panel).astype(jnp.float32)
        if layer_index == 0:
            product = jnp.einsum('ikc,jkc->cij', left_panel, right_panel)
        else:
            product = jnp.einsum('kic,kjc->cij', left_panel, right_panel)
        return product.astype(jnp.bfloat16)
    groups = jnp.arange(CH // group_width, dtype=jnp.int32)
    product = lax.map(channel_group, groups).reshape(CH, NTOK, NTOK)
    normed = normalize(product.astype(jnp.float32), output_gain[layer_index][:, None, None], output_bias[layer_index][:, None, None], 0)
    normed = lax.optimization_barrier(normed.astype(jnp.bfloat16)).astype(jnp.float32)
    update = jnp.einsum('cij,cd->ijd', normed, output_weights[layer_index].astype(jnp.float32))
    return current + gate_value * update

def reference(pair_state, pair_mask, input_gain, input_bias, proj_weights, gate_weights, output_gain, output_bias, output_weights):
    current = pair_state.astype(jnp.float32)
    mask_float = pair_mask.astype(jnp.float32)[:, :, None]
    for layer_index in range(2):
        current = triangle(current, mask_float, layer_index, input_gain, input_bias, proj_weights, gate_weights, output_gain, output_bias, output_weights)
    return current.astype(jnp.bfloat16)
```

```python
import functools

import jax
import jax.numpy as jnp
from jax import lax
from jax.experimental import pallas as pl
from jax.experimental.pallas import tpu as pltpu
from jax.sharding import PartitionSpec as P

epsilon = 1e-05


def normalize(values, weight_scale, weight_shift, reduce_axis):
    average = jnp.mean(values, axis=reduce_axis, keepdims=True)
    centred = values - average
    spread = jnp.mean(centred * centred, axis=reduce_axis, keepdims=True)
    return centred * lax.rsqrt(spread + epsilon) * weight_scale + weight_shift


def contract(left_panel, right_panel, layer_index):
    if layer_index == 0:
        product = jnp.einsum(
            "cik,cjk->cij", left_panel, right_panel, preferred_element_type=jnp.float32
        )
    else:
        product = jnp.einsum(
            "cki,ckj->cij", left_panel, right_panel, preferred_element_type=jnp.float32
        )
    return product.astype(jnp.bfloat16)


def gated_panel(pair_ln, weights, first, hidden, mask_float):
    projected = jnp.einsum(
        "ijd,de->eij",
        pair_ln,
        weights[:, first : first + 2 * hidden],
        preferred_element_type=jnp.float32,
    )
    return (jax.nn.sigmoid(projected[:hidden]) * projected[hidden:] * mask_float).astype(
        jnp.bfloat16
    )


def on_device(
    pair_state,
    pair_mask,
    input_gain,
    input_bias,
    proj_weights,
    gate_weights,
    output_gain,
    output_bias,
    output_weights,
):
    tile_rows, tile_cols, channels = pair_state.shape
    hidden = output_weights.shape[1]
    row_count = lax.axis_size("row")
    col_count = lax.axis_size("col")
    per_device = hidden // (row_count * col_count)
    current = pair_state.astype(jnp.float32)
    mask_float = pair_mask.astype(jnp.float32)[None]
    for layer_index in range(2):
        pair_ln = normalize(current, input_gain[layer_index], input_bias[layer_index], -1).astype(
            jnp.bfloat16
        )
        left_panel = gated_panel(pair_ln, proj_weights[layer_index], 0, hidden, mask_float)
        right_panel = gated_panel(
            pair_ln, proj_weights[layer_index], 2 * hidden, hidden, mask_float
        )
        gate_value = jax.nn.sigmoid(
            jnp.einsum(
                "ijd,de->ije",
                pair_ln,
                gate_weights[layer_index],
                preferred_element_type=jnp.float32,
            )
        )
        scale_out = output_gain[layer_index]
        shift_out = output_bias[layer_index]
        weight_out = output_weights[layer_index]
        left_recv, right_recv = (
            lax.all_to_all(left_panel, ("row", "col"), split_axis=0, concat_axis=1, tiled=True),
            lax.all_to_all(right_panel, ("row", "col"), split_axis=0, concat_axis=1, tiled=True),
        )
        left_chan = (
            left_recv.reshape(per_device, row_count, col_count, tile_rows, tile_cols)
            .transpose(0, 1, 3, 2, 4)
            .reshape(per_device, row_count * tile_rows, col_count * tile_cols)
        )
        right_chan = (
            right_recv.reshape(per_device, row_count, col_count, tile_rows, tile_cols)
            .transpose(0, 1, 3, 2, 4)
            .reshape(per_device, row_count * tile_rows, col_count * tile_cols)
        )
        product = contract(left_chan, right_chan, layer_index)
        arranged = (
            product.reshape(per_device, row_count, tile_rows, col_count, tile_cols)
            .transpose(0, 1, 3, 2, 4)
            .reshape(per_device, row_count * col_count * tile_rows, tile_cols)
        )
        returned = lax.all_to_all(arranged, ("row", "col"), split_axis=1, concat_axis=0, tiled=True)
        normed = normalize(
            returned.astype(jnp.float32), scale_out[:, None, None], shift_out[:, None, None], 0
        ).astype(jnp.bfloat16)
        update = jnp.einsum("cij,cd->ijd", normed, weight_out, preferred_element_type=jnp.float32)
        current = current + gate_value * update
    return current.astype(jnp.bfloat16)


MESH = pl.DeviceIdType.MESH
F32 = jnp.float32
BF16 = jnp.bfloat16
CHUNKS = 2


def sigmoid(values):
    return 0.5 * jnp.tanh(0.5 * values) + 0.5


def lane_groups(shape, width):
    return lax.broadcasted_iota(jnp.int32, shape, len(shape) - 1) // width


def swap_groups(blocks, width):
    count = len(blocks)
    blocks = list(blocks)
    lanes = count * width
    group = lane_groups(blocks[0].shape, width)
    step = count // 2
    while step:
        low = (group // step) % 2 == 0
        for p in range(count):
            if p & step:
                continue
            first, second = blocks[p], blocks[p + step]
            shift = step * width
            blocks[p] = jnp.where(low, first, pltpu.roll(second, shift, 1))
            blocks[p + step] = jnp.where(low, pltpu.roll(first, lanes - shift, 1), second)
        step //= 2
    return blocks


def columns_of(row_vector, lanes):
    return jnp.transpose(jnp.broadcast_to(row_vector, (lanes, row_vector.shape[1])))


def contract_first(left, right):
    return lax.dot_general(left, right, (((0,), (0,)), ((), ())), preferred_element_type=F32)


def fused_kernel(row_count, col_count, *refs):
    operands, out_ref, held = refs[:9], refs[9], refs[10:19]
    load_sem = refs[19]
    loads = [
        pltpu.make_async_copy(source, target, load_sem.at[at])
        for at, (source, target) in enumerate(zip(operands, held))
    ]
    for at in (0, 4, 2, 3, 1, 5, 6, 7, 8):
        loads[at].start()
    fused_body(row_count, col_count, loads, *held, out_ref, *refs[20:])


def fused_body(
    row_count,
    col_count,
    loads,
    z_ref,
    mask_ref,
    in_gain,
    in_bias,
    proj_ref,
    gate_ref,
    out_gain,
    out_bias,
    outw_ref,
    out_ref,
    zt_ref,
    tmp_ref,
    gated_ref,
    in_gain_ref,
    in_bias_ref,
    gain_ref,
    bias_ref,
    send1,
    recv_k,
    recv_a,
    recv_b,
    send_sum,
    recv_sum,
    send_own,
    recv_own,
    send_sem,
    recv_sem,
):
    tile_rows, tile_cols, channels = z_ref.shape
    devices = row_count * col_count
    hidden = outw_ref.shape[1]
    half = col_count // 2
    width = tile_cols // CHUNKS
    pairs = tile_rows * width
    owners = row_count * half
    own = hidden // owners
    lanes = own * width
    blocks = pairs // lanes
    tokens = row_count * tile_rows
    row, col = lax.axis_index("row"), lax.axis_index("col")
    near, inner = col // half, lax.rem(col, half)
    me = row * half + inner

    def place(turn, step):
        if turn < half:
            tcol = (1 - near) * half + lax.rem(2 * half - 1 - inner + turn, half)
            trow = lax.rem(2 * row_count - 1 - row + step, row_count)
        else:
            tcol = near * half + lax.rem(inner + 1 + turn - half, half)
            trow = lax.rem(row + 1 + step, row_count)
        return trow, tcol

    def each(action, first=0):
        for turn in range(first, col_count):

            def body(step, carry, turn=turn):
                action(*place(turn, step))
                return carry

            lax.fori_loop(0, row_count - (turn == col_count - 1), body, 0, unroll=True)

    barrier = pltpu.get_barrier_semaphore()

    def greet(trow, tcol):
        pl.semaphore_signal(barrier, inc=1, device_id=(trow, tcol), device_id_type=MESH)

    each(greet)

    def send(source, target, at, trow, tcol):
        pltpu.make_async_remote_copy(
            src_ref=source,
            dst_ref=target,
            send_sem=send_sem.at[at],
            recv_sem=recv_sem.at[at],
            device_id=(trow, tcol),
            device_id_type=MESH,
        ).start()

    def owner(trow, tcol):
        return trow * half + lax.rem(tcol, half)

    slot = inner * row_count + row

    def start_k(chunk):
        each(
            lambda trow, tcol: send(
                send1.at[0, chunk, owner(trow, tcol)], recv_k.at[chunk, slot], chunk, trow, tcol
            ),
            half,
        )
        recv_k[chunk, slot] = send1[0, chunk, me]

    def wait_k(sem, chunk):
        slots = recv_k.at[chunk, pl.ds(0, owners - 1)]
        pltpu.make_async_copy(slots, slots, sem.at[chunk]).wait()

    def start_sum(chunk):
        each(
            lambda trow, tcol: send(
                send_sum.at[chunk, tcol, trow],
                recv_sum.at[chunk, near * owners + me],
                CHUNKS + chunk,
                trow,
                tcol,
            )
        )
        recv_sum[chunk, near * owners + me] = send_sum[chunk, col, row]

    def wait_sum(sem, chunk):
        slots = recv_sum.at[chunk, pl.ds(0, devices - 1)]
        pltpu.make_async_copy(slots, slots, sem.at[CHUNKS + chunk]).wait()

    def start_ab(chunk):
        each(
            lambda trow, tcol: send(
                send1.at[1, chunk, owner(trow, tcol), 0],
                recv_a.at[chunk, col * row_count + row],
                2 * CHUNKS + chunk,
                trow,
                tcol,
            )
        )
        each(
            lambda trow, tcol: send(
                send1.at[1, chunk, owner(trow, tcol), 1],
                recv_b.at[chunk, slot],
                3 * CHUNKS + chunk,
                trow,
                tcol,
            ),
            half,
        )
        recv_a[chunk, col * row_count + row] = send1[1, chunk, me, 0]
        recv_b[chunk, slot] = send1[1, chunk, me, 1]

    def wait_ab(sem, chunk):
        slots = recv_a.at[chunk, pl.ds(0, devices - 1)]
        pltpu.make_async_copy(slots, slots, sem.at[2 * CHUNKS + chunk]).wait()
        slots = recv_b.at[chunk, pl.ds(0, owners - 1)]
        pltpu.make_async_copy(slots, slots, sem.at[3 * CHUNKS + chunk]).wait()

    def start_own(chunk):
        each(
            lambda trow, tcol: send(
                send_own.at[chunk, lax.rem(tcol, half), trow],
                recv_own.at[chunk, me],
                4 * CHUNKS + chunk,
                trow,
                tcol,
            ),
            half,
        )
        recv_own[chunk, me] = send_own[chunk, inner, row]

    def wait_own(sem, chunk):
        slots = recv_own.at[chunk, pl.ds(0, owners - 1)]
        pltpu.make_async_copy(slots, slots, sem.at[4 * CHUNKS + chunk]).wait()

    def spread_inputs(layer):
        in_gain_ref[layer] = columns_of(in_gain[layer : layer + 1, :], lanes)
        in_bias_ref[layer] = columns_of(in_bias[layer : layer + 1, :], lanes)

    def spread_outputs(layer):
        group = lane_groups((owners, lanes), width)
        for source, kept in ((out_gain, gain_ref), (out_bias, bias_ref)):
            wide = columns_of(source[layer : layer + 1, :], lanes)
            packed = wide[0:owners]
            for k in range(1, own):
                packed = jnp.where(group == k, wide[k * owners : (k + 1) * owners], packed)
            kept[layer] = packed

    def front(layer, chunk, current, mask_flat):
        centred = current - jnp.mean(current, axis=0, keepdims=True)
        scale = lax.rsqrt(jnp.mean(centred * centred, axis=0, keepdims=True) + epsilon)
        gain = jnp.concatenate([in_gain_ref[layer]] * blocks, axis=1)
        bias = jnp.concatenate([in_bias_ref[layer]] * blocks, axis=1)
        normed = (centred * scale * gain + bias).astype(BF16)
        projected = contract_first(proj_ref[layer], normed)
        for side in range(2):
            first = 2 * side * hidden
            panel = (
                sigmoid(projected[first : first + hidden])
                * projected[first + hidden : first + 2 * hidden]
                * mask_flat
            )
            for block in range(blocks):
                parts = [
                    panel[k * owners : (k + 1) * owners, block * lanes : (block + 1) * lanes]
                    for k in range(own)
                ]
                for q, part in enumerate(swap_groups(parts, width)):
                    line = block * own + q
                    tmp_ref[side, line * owners : (line + 1) * owners, :] = part
            for target in range(owners):
                send1[layer, chunk, target, side] = tmp_ref[
                    side, pl.ds(target, tile_rows, stride=owners), :
                ].astype(BF16)
        return normed

    def gate(layer, chunk, normed):
        gated_ref[chunk] = sigmoid(contract_first(gate_ref[layer], normed))

    def over_channels(values):
        total = jnp.sum(values, axis=0)
        shift = lanes // 2
        while shift >= width:
            total = total + pltpu.roll(total, shift, 1)
            shift //= 2
        return total * (1.0 / hidden)

    def back(layer, chunk, returned):
        centred = returned - over_channels(returned)[None]
        scale = lax.rsqrt(over_channels(centred * centred) + epsilon)
        for d in range(owners):
            tmp_ref[0, d * tile_rows : (d + 1) * tile_rows, :] = (
                centred[d] * scale * gain_ref[layer, d : d + 1, :] + bias_ref[layer, d : d + 1, :]
            )
        wide_blocks = []
        for block in range(blocks):
            parts = [
                tmp_ref[0, pl.ds(block * own + q, owners, stride=tile_rows), :] for q in range(own)
            ]
            wide_blocks.append(jnp.concatenate(swap_groups(parts, width), axis=0).astype(BF16))
        update = contract_first(outw_ref[layer], jnp.concatenate(wide_blocks, axis=1))
        return zt_ref[chunk] + gated_ref[chunk] * update

    for at in (2, 3):
        loads[at].wait()
    spread_inputs(0)
    loads[1].wait()
    mask_float = mask_ref[...].astype(F32)
    across = lax.broadcasted_iota(jnp.int32, (tile_cols, pairs), 1) % width
    mine = (
        lax.broadcasted_iota(jnp.int32, (tile_rows, pairs), 1) // width
        == lax.broadcasted_iota(jnp.int32, (tile_rows, pairs), 0)
    ).astype(F32)
    mask_flat = []
    for chunk in range(CHUNKS):
        spread = (
            across + chunk * width == lax.broadcasted_iota(jnp.int32, (tile_cols, pairs), 0)
        ).astype(F32)
        mask_flat.append(
            jnp.sum(
                jnp.dot(mask_float, spread, preferred_element_type=F32) * mine,
                axis=0,
                keepdims=True,
            )
        )
    loads[0].wait()
    loads[4].wait()
    normed = [None] * CHUNKS
    for chunk in range(CHUNKS):
        zt_ref[chunk] = jnp.transpose(
            z_ref[:, chunk * width : (chunk + 1) * width, :].astype(F32).reshape(pairs, channels)
        )
        normed[chunk] = front(0, chunk, zt_ref[chunk], mask_flat[chunk])
        if chunk == 0:
            pl.semaphore_wait(barrier, devices - 1)
        start_k(chunk)
    for at in (5, 6, 7, 8):
        loads[at].wait()
    for chunk in range(CHUNKS):
        gate(0, chunk, normed[chunk])
    spread_inputs(1)
    for layer in range(2):
        spread_outputs(layer)
    for chunk in range(CHUNKS):
        wait_k(recv_sem, chunk)

    def panel(ref, chunk, plane, *side):
        return ref[
            (chunk, slice(plane * row_count, (plane + 1) * row_count)) + side
        ].reshape(tokens, lanes)

    spans = [(chunk, plane) for chunk in range(CHUNKS) for plane in range(half)]
    left = jnp.concatenate([panel(recv_k, c, p, 0) for c, p in spans], axis=1)
    right = jnp.concatenate([panel(recv_k, c, p, 1) for c, p in spans], axis=1)
    lane_group = lane_groups((1, len(spans) * lanes), width) % own
    masks = [(lane_group == k).astype(F32).astype(BF16) for k in range(own)]
    for chunk in range(CHUNKS):
        for c in range(col_count):
            at = (c * CHUNKS + chunk) * width
            rows = right[at : at + width]
            stacked = jnp.concatenate([rows * masks[k] for k in range(own)], axis=0)
            product = lax.dot_general(
                left, stacked, (((1,), (1,)), ((), ())), preferred_element_type=F32
            )
            send_sum[chunk, c] = product.astype(BF16).reshape(row_count, tile_rows, lanes)
        start_sum(chunk)

    for chunk in range(CHUNKS):
        wait_sum(recv_sem, chunk)
        returned = recv_sum[chunk, 0:owners].astype(F32) + recv_sum[
            chunk, owners : 2 * owners
        ].astype(F32)
        zt_ref[chunk] = back(0, chunk, returned)
        normed[chunk] = front(1, chunk, zt_ref[chunk], mask_flat[chunk])
        start_ab(chunk)
    for chunk in range(CHUNKS):
        gate(1, chunk, normed[chunk])
    for chunk in range(CHUNKS):
        wait_ab(recv_sem, chunk)

    left = jnp.concatenate(
        [panel(recv_a, chunk, c) for c in range(col_count) for chunk in range(CHUNKS)], axis=1
    )
    group = lane_groups((width, lanes), width)
    for chunk in range(CHUNKS):
        right = jnp.concatenate([panel(recv_b, chunk, p) for p in range(half)], axis=1)
        product = contract_first(left, right)
        for p in range(half):
            for r in range(row_count):
                at = r * lanes
                piece = product[at : at + width, p * lanes : (p + 1) * lanes]
                for k in range(1, own):
                    low = at + k * width
                    piece = jnp.where(
                        group == k,
                        product[low : low + width, p * lanes : (p + 1) * lanes],
                        piece,
                    )
                send_own[chunk, p, r] = piece.astype(BF16)
        start_own(chunk)

    for chunk in range(CHUNKS):
        wait_own(recv_sem, chunk)
        final = back(1, chunk, recv_own[chunk].astype(F32))
        out_ref[:, chunk * width : (chunk + 1) * width, :] = (
            jnp.transpose(final).reshape(tile_rows, width, channels).astype(BF16)
        )
    for chunk in range(CHUNKS):
        wait_k(send_sem, chunk)
        wait_sum(send_sem, chunk)
        wait_ab(send_sem, chunk)
        wait_own(send_sem, chunk)


def fused(row_count, col_count, *args):
    tile_rows, tile_cols, channels = args[0].shape
    devices = row_count * col_count
    hidden = args[-1].shape[1]
    half = col_count // 2
    owners = row_count * half
    width = tile_cols // CHUNKS
    lanes = hidden // owners * width
    pairs = tile_rows * width
    vmem = pl.BlockSpec(memory_space=pltpu.VMEM)
    return pl.pallas_call(
        functools.partial(fused_kernel, row_count, col_count),
        out_shape=jax.ShapeDtypeStruct(args[0].shape, BF16),
        in_specs=[pl.BlockSpec(memory_space=pl.ANY)] * len(args),
        out_specs=vmem,
        scratch_shapes=[pltpu.VMEM(arg.shape, arg.dtype) for arg in args]
        + [
            pltpu.SemaphoreType.DMA((len(args),)),
            pltpu.VMEM((CHUNKS, channels, pairs), F32),
            pltpu.VMEM((2, tile_rows * owners, lanes), F32),
            pltpu.VMEM((CHUNKS, channels, pairs), F32),
            pltpu.VMEM((2, channels, lanes), F32),
            pltpu.VMEM((2, channels, lanes), F32),
            pltpu.VMEM((2, owners, lanes), F32),
            pltpu.VMEM((2, owners, lanes), F32),
            pltpu.VMEM((2, CHUNKS, owners, 2, tile_rows, lanes), BF16),
            pltpu.VMEM((CHUNKS, owners, 2, tile_rows, lanes), BF16),
            pltpu.VMEM((CHUNKS, devices, tile_rows, lanes), BF16),
            pltpu.VMEM((CHUNKS, owners, tile_rows, lanes), BF16),
            pltpu.VMEM((CHUNKS, col_count, row_count, tile_rows, lanes), BF16),
            pltpu.VMEM((CHUNKS, devices, tile_rows, lanes), BF16),
            pltpu.VMEM((CHUNKS, half, row_count, tile_rows, lanes), BF16),
            pltpu.VMEM((CHUNKS, owners, tile_rows, lanes), BF16),
            pltpu.SemaphoreType.DMA((5 * CHUNKS,)),
            pltpu.SemaphoreType.DMA((5 * CHUNKS,)),
        ],
        compiler_params=pltpu.CompilerParams(collective_id=0, has_side_effects=True),
    )(*args)


def solution(mesh):
    row_count, col_count = mesh.shape["row"], mesh.shape["col"]
    devices = row_count * col_count

    def step(*args):
        tile_rows, tile_cols, channels = args[0].shape
        hidden = args[-1].shape[1]
        owners = devices // 2
        own = hidden // owners
        width = tile_cols // CHUNKS
        fits = (
            hidden % devices == 0
            and col_count % 2 == 0
            and tile_cols % CHUNKS == 0
            and own * width == 128
            and tile_rows == width
            and tile_rows % 16 == 0
            and tile_rows % own == 0
            and own & (own - 1) == 0
            and row_count * tile_rows == col_count * tile_cols
        )
        return fused(row_count, col_count, *args) if fits else on_device(*args)

    return jax.shard_map(
        step,
        mesh=mesh,
        in_specs=(P("row", "col", None), P("row", "col"), P(), P(), P(), P(), P(), P(), P()),
        out_specs=P("row", "col", None),
        check_vma=False,
    )
```

```python
import functools

import jax
import jax.numpy as jnp
from jax import lax
from jax.experimental import pallas as pl
from jax.experimental.pallas import tpu as pltpu
from jax.sharding import PartitionSpec as P

epsilon = 1e-05


def normalize(values, weight_scale, weight_shift, reduce_axis):
    average = jnp.mean(values, axis=reduce_axis, keepdims=True)
    centred = values - average
    spread = jnp.mean(centred * centred, axis=reduce_axis, keepdims=True)
    return centred * lax.rsqrt(spread + epsilon) * weight_scale + weight_shift


def contract(left_panel, right_panel, layer_index):
    if layer_index == 0:
        product = jnp.einsum(
            "cik,cjk->cij", left_panel, right_panel, preferred_element_type=jnp.float32
        )
    else:
        product = jnp.einsum(
            "cki,ckj->cij", left_panel, right_panel, preferred_element_type=jnp.float32
        )
    return product.astype(jnp.bfloat16)


def gated_panel(pair_ln, weights, first, hidden, mask_float):
    projected = jnp.einsum(
        "ijd,de->eij",
        pair_ln,
        weights[:, first : first + 2 * hidden],
        preferred_element_type=jnp.float32,
    )
    return (jax.nn.sigmoid(projected[:hidden]) * projected[hidden:] * mask_float).astype(
        jnp.bfloat16
    )


def on_device(
    pair_state,
    pair_mask,
    input_gain,
    input_bias,
    proj_weights,
    gate_weights,
    output_gain,
    output_bias,
    output_weights,
):
    tile_rows, tile_cols, channels = pair_state.shape
    hidden = output_weights.shape[1]
    row_count = lax.axis_size("row")
    col_count = lax.axis_size("col")
    per_device = hidden // (row_count * col_count)
    current = pair_state.astype(jnp.float32)
    mask_float = pair_mask.astype(jnp.float32)[None]
    for layer_index in range(2):
        pair_ln = normalize(current, input_gain[layer_index], input_bias[layer_index], -1).astype(
            jnp.bfloat16
        )
        left_panel = gated_panel(pair_ln, proj_weights[layer_index], 0, hidden, mask_float)
        right_panel = gated_panel(
            pair_ln, proj_weights[layer_index], 2 * hidden, hidden, mask_float
        )
        gate_value = jax.nn.sigmoid(
            jnp.einsum(
                "ijd,de->ije",
                pair_ln,
                gate_weights[layer_index],
                preferred_element_type=jnp.float32,
            )
        )
        scale_out = output_gain[layer_index]
        shift_out = output_bias[layer_index]
        weight_out = output_weights[layer_index]
        left_recv, right_recv = (
            lax.all_to_all(left_panel, ("row", "col"), split_axis=0, concat_axis=1, tiled=True),
            lax.all_to_all(right_panel, ("row", "col"), split_axis=0, concat_axis=1, tiled=True),
        )
        left_chan = (
            left_recv.reshape(per_device, row_count, col_count, tile_rows, tile_cols)
            .transpose(0, 1, 3, 2, 4)
            .reshape(per_device, row_count * tile_rows, col_count * tile_cols)
        )
        right_chan = (
            right_recv.reshape(per_device, row_count, col_count, tile_rows, tile_cols)
            .transpose(0, 1, 3, 2, 4)
            .reshape(per_device, row_count * tile_rows, col_count * tile_cols)
        )
        product = contract(left_chan, right_chan, layer_index)
        arranged = (
            product.reshape(per_device, row_count, tile_rows, col_count, tile_cols)
            .transpose(0, 1, 3, 2, 4)
            .reshape(per_device, row_count * col_count * tile_rows, tile_cols)
        )
        returned = lax.all_to_all(arranged, ("row", "col"), split_axis=1, concat_axis=0, tiled=True)
        normed = normalize(
            returned.astype(jnp.float32), scale_out[:, None, None], shift_out[:, None, None], 0
        ).astype(jnp.bfloat16)
        update = jnp.einsum("cij,cd->ijd", normed, weight_out, preferred_element_type=jnp.float32)
        current = current + gate_value * update
    return current.astype(jnp.bfloat16)


MESH = pl.DeviceIdType.MESH
F32 = jnp.float32
BF16 = jnp.bfloat16
CHUNKS = 2


def sigmoid(values):
    return 0.5 * jnp.tanh(0.5 * values) + 0.5


def lane_groups(shape, width):
    return lax.broadcasted_iota(jnp.int32, shape, len(shape) - 1) // width


def swap_groups(blocks, width):
    count = len(blocks)
    blocks = list(blocks)
    lanes = count * width
    group = lane_groups(blocks[0].shape, width)
    step = count // 2
    while step:
        low = (group // step) % 2 == 0
        for p in range(count):
            if p & step:
                continue
            first, second = blocks[p], blocks[p + step]
            shift = step * width
            blocks[p] = jnp.where(low, first, pltpu.roll(second, shift, 1))
            blocks[p + step] = jnp.where(low, pltpu.roll(first, lanes - shift, 1), second)
        step //= 2
    return blocks


def columns_of(row_vector, lanes):
    return jnp.transpose(jnp.broadcast_to(row_vector, (lanes, row_vector.shape[1])))


def contract_first(left, right):
    return lax.dot_general(left, right, (((0,), (0,)), ((), ())), preferred_element_type=F32)


def fused_kernel(row_count, col_count, *refs):
    operands, out_ref, held = refs[:9], refs[9], refs[10:19]
    load_sem = refs[19]
    loads = [
        pltpu.make_async_copy(source, target, load_sem.at[at])
        for at, (source, target) in enumerate(zip(operands, held))
    ]
    for at in (0, 4, 2, 3, 1, 5, 6, 7, 8):
        loads[at].start()
    fused_body(row_count, col_count, loads, *held, out_ref, *refs[20:])


def fused_body(
    row_count,
    col_count,
    loads,
    z_ref,
    mask_ref,
    in_gain,
    in_bias,
    proj_ref,
    gate_ref,
    out_gain,
    out_bias,
    outw_ref,
    out_ref,
    zt_ref,
    tmp_ref,
    gated_ref,
    in_gain_ref,
    in_bias_ref,
    gain_ref,
    bias_ref,
    send_k,
    recv_k,
    send_ab,
    recv_a,
    recv_ab,
    send_sum,
    recv_sum,
    send_own,
    recv_own,
    send_sem,
    recv_sem,
):
    tile_rows, tile_cols, channels = z_ref.shape
    devices = row_count * col_count
    hidden = outw_ref.shape[1]
    half = col_count // 2
    width = tile_cols // CHUNKS
    pairs = tile_rows * width
    owners = row_count * half
    own = hidden // owners
    lanes = own * width
    blocks = pairs // lanes
    tokens = row_count * tile_rows
    row, col = lax.axis_index("row"), lax.axis_index("col")
    near, inner = col // half, lax.rem(col, half)
    me = row * half + inner

    def flips(index, count):
        bits = count.bit_length() - 1
        moves = [(1 << b) * (1 - 2 * lax.rem(index // (1 << b), 2)) for b in range(bits)]

        def flipped(pattern):
            total = index
            for b in range(bits):
                if pattern >> b & 1:
                    total = total + moves[b]
            return total

        return [flipped(pattern) for pattern in range(count)]

    rows, cols = flips(row, row_count), flips(col, col_count)
    row_order = sorted(range(row_count), key=lambda p: (-p.bit_count(), -p))
    across = list(range(half, col_count))
    within = list(range(half - 1, -1, -1))

    def each(action, turns):
        for turn in turns:
            for step in row_order:
                if turn or step:
                    action(rows[step], cols[turn])

    barrier = pltpu.get_barrier_semaphore()

    def greet(trow, tcol):
        pl.semaphore_signal(barrier, inc=1, device_id=(trow, tcol), device_id_type=MESH)

    each(greet, across + within)

    def send(source, target, at, trow, tcol):
        pltpu.make_async_remote_copy(
            src_ref=source,
            dst_ref=target,
            send_sem=send_sem.at[at],
            recv_sem=recv_sem.at[at],
            device_id=(trow, tcol),
            device_id_type=MESH,
        ).start()

    def owner(trow, tcol):
        return trow * half + lax.rem(tcol, half)

    slot = inner * row_count + row

    def start_k():
        each(
            lambda trow, tcol: send(send_k.at[owner(trow, tcol)], recv_k.at[slot], 0, trow, tcol),
            within,
        )
        recv_k[slot] = send_k[me]

    def wait_k(sem):
        slots = recv_k.at[pl.ds(0, owners - 1)]
        pltpu.make_async_copy(slots, slots, sem.at[0]).wait()

    def start_sum(chunk):
        each(
            lambda trow, tcol: send(
                send_sum.at[chunk, tcol, trow],
                recv_sum.at[chunk, near * owners + me],
                CHUNKS + chunk,
                trow,
                tcol,
            ),
            across + within,
        )
        recv_sum[chunk, near * owners + me] = send_sum[chunk, col, row]

    def wait_sum(sem, chunk):
        slots = recv_sum.at[chunk, pl.ds(0, devices - 1)]
        pltpu.make_async_copy(slots, slots, sem.at[CHUNKS + chunk]).wait()

    def start_ab(chunk):
        each(
            lambda trow, tcol: send(
                send_ab.at[chunk, owner(trow, tcol), 0],
                recv_a.at[chunk, slot],
                2 * CHUNKS + chunk,
                trow,
                tcol,
            ),
            across,
        )
        each(
            lambda trow, tcol: send(
                send_ab.at[chunk, owner(trow, tcol)],
                recv_ab.at[chunk, slot],
                3 * CHUNKS + chunk,
                trow,
                tcol,
            ),
            within,
        )
        recv_ab[chunk, slot] = send_ab[chunk, me]

    def wait_ab(sem, chunk):
        slots = recv_a.at[chunk]
        pltpu.make_async_copy(slots, slots, sem.at[2 * CHUNKS + chunk]).wait()
        slots = recv_ab.at[chunk, pl.ds(0, owners - 1)]
        pltpu.make_async_copy(slots, slots, sem.at[3 * CHUNKS + chunk]).wait()

    def start_own(chunk):
        each(
            lambda trow, tcol: send(
                send_own.at[chunk, lax.rem(tcol, half), trow],
                recv_own.at[chunk, me],
                4 * CHUNKS + chunk,
                trow,
                tcol,
            ),
            within,
        )
        recv_own[chunk, me] = send_own[chunk, inner, row]

    def wait_own(sem, chunk):
        slots = recv_own.at[chunk, pl.ds(0, owners - 1)]
        pltpu.make_async_copy(slots, slots, sem.at[4 * CHUNKS + chunk]).wait()

    def spread_inputs(layer):
        in_gain_ref[layer] = columns_of(in_gain[layer : layer + 1, :], lanes)
        in_bias_ref[layer] = columns_of(in_bias[layer : layer + 1, :], lanes)

    def spread_outputs(layer):
        group = lane_groups((owners, lanes), width)
        for source, kept in ((out_gain, gain_ref), (out_bias, bias_ref)):
            wide = columns_of(source[layer : layer + 1, :], lanes)
            packed = wide[0:owners]
            for k in range(1, own):
                packed = jnp.where(group == k, wide[k * owners : (k + 1) * owners], packed)
            kept[layer] = packed

    def front(layer, chunk, current, mask_flat, target_at):
        centred = current - jnp.mean(current, axis=0, keepdims=True)
        scale = lax.rsqrt(jnp.mean(centred * centred, axis=0, keepdims=True) + epsilon)
        gain = jnp.concatenate([in_gain_ref[layer]] * blocks, axis=1)
        bias = jnp.concatenate([in_bias_ref[layer]] * blocks, axis=1)
        normed = (centred * scale * gain + bias).astype(BF16)
        projected = contract_first(proj_ref[layer], normed)
        for side in range(2):
            first = 2 * side * hidden
            panel = (
                sigmoid(projected[first : first + hidden])
                * projected[first + hidden : first + 2 * hidden]
                * mask_flat
            )
            for block in range(blocks):
                parts = [
                    panel[k * owners : (k + 1) * owners, block * lanes : (block + 1) * lanes]
                    for k in range(own)
                ]
                for q, part in enumerate(swap_groups(parts, width)):
                    line = block * own + q
                    tmp_ref[side, line * owners : (line + 1) * owners, :] = part
            for target in range(owners):
                target_at(target)[side] = tmp_ref[
                    side, pl.ds(target, tile_rows, stride=owners), :
                ].astype(BF16)
        return normed

    def gate(layer, chunk, normed):
        gated_ref[chunk] = sigmoid(contract_first(gate_ref[layer], normed))

    def over_channels(values):
        total = jnp.sum(values, axis=0)
        shift = lanes // 2
        while shift >= width:
            total = total + pltpu.roll(total, shift, 1)
            shift //= 2
        return total * (1.0 / hidden)

    def back(layer, chunk, returned):
        centred = returned - over_channels(returned)[None]
        scale = lax.rsqrt(over_channels(centred * centred) + epsilon)
        for d in range(owners):
            tmp_ref[0, d * tile_rows : (d + 1) * tile_rows, :] = (
                centred[d] * scale * gain_ref[layer, d : d + 1, :] + bias_ref[layer, d : d + 1, :]
            )
        wide_blocks = []
        for block in range(blocks):
            parts = [
                tmp_ref[0, pl.ds(block * own + q, owners, stride=tile_rows), :] for q in range(own)
            ]
            wide_blocks.append(jnp.concatenate(swap_groups(parts, width), axis=0).astype(BF16))
        update = contract_first(outw_ref[layer], jnp.concatenate(wide_blocks, axis=1))
        return zt_ref[chunk] + gated_ref[chunk] * update

    for at in (2, 3):
        loads[at].wait()
    spread_inputs(0)
    loads[1].wait()
    mask_float = mask_ref[...].astype(F32)
    column = lax.broadcasted_iota(jnp.int32, (tile_cols, pairs), 1) % width
    mine = (
        lax.broadcasted_iota(jnp.int32, (tile_rows, pairs), 1) // width
        == lax.broadcasted_iota(jnp.int32, (tile_rows, pairs), 0)
    ).astype(F32)
    mask_flat = []
    for chunk in range(CHUNKS):
        spread = (
            column + chunk * width == lax.broadcasted_iota(jnp.int32, (tile_cols, pairs), 0)
        ).astype(F32)
        mask_flat.append(
            jnp.sum(
                jnp.dot(mask_float, spread, preferred_element_type=F32) * mine,
                axis=0,
                keepdims=True,
            )
        )
    loads[0].wait()
    loads[4].wait()
    normed = [None] * CHUNKS
    for chunk in range(CHUNKS):
        zt_ref[chunk] = jnp.transpose(
            z_ref[:, chunk * width : (chunk + 1) * width, :].astype(F32).reshape(pairs, channels)
        )
        normed[chunk] = front(
            0,
            chunk,
            zt_ref[chunk],
            mask_flat[chunk],
            lambda target, chunk=chunk: send_k.at[target, chunk],
        )
    for at in (5, 6, 7, 8):
        loads[at].wait()
    for chunk in range(CHUNKS):
        gate(0, chunk, normed[chunk])
    spread_inputs(1)
    for layer in range(2):
        spread_outputs(layer)
    pl.semaphore_wait(barrier, devices - 1)
    start_k()
    wait_k(recv_sem)

    def panel(ref, plane, *at):
        span = (slice(plane * row_count, (plane + 1) * row_count),)
        return ref[at[:1] + span + at[1:] if ref is not recv_k else span + at].reshape(tokens, lanes)

    spans = [(chunk, plane) for chunk in range(CHUNKS) for plane in range(half)]
    left = jnp.concatenate([panel(recv_k, p, c, 0) for c, p in spans], axis=1)
    right = jnp.concatenate([panel(recv_k, p, c, 1) for c, p in spans], axis=1)
    lane_group = lane_groups((1, len(spans) * lanes), width) % own
    masks = [(lane_group == k).astype(F32).astype(BF16) for k in range(own)]
    for chunk in range(CHUNKS):
        for c in range(col_count):
            at = (c * CHUNKS + chunk) * width
            lines = right[at : at + width]
            stacked = jnp.concatenate([lines * masks[k] for k in range(own)], axis=0)
            product = lax.dot_general(
                left, stacked, (((1,), (1,)), ((), ())), preferred_element_type=F32
            )
            send_sum[chunk, c] = product.astype(BF16).reshape(row_count, tile_rows, lanes)
        start_sum(chunk)

    for chunk in range(CHUNKS):
        wait_sum(recv_sem, chunk)
        returned = recv_sum[chunk, 0:owners].astype(F32) + recv_sum[
            chunk, owners : 2 * owners
        ].astype(F32)
        zt_ref[chunk] = back(0, chunk, returned)
        normed[chunk] = front(
            1,
            chunk,
            zt_ref[chunk],
            mask_flat[chunk],
            lambda target, chunk=chunk: send_ab.at[chunk, target],
        )
        start_ab(chunk)
    for chunk in range(CHUNKS):
        gate(1, chunk, normed[chunk])
    group = lane_groups((width, lanes), width)

    def pieces(left_chunk, chunk):
        right = jnp.concatenate([panel(recv_ab, p, chunk, 1) for p in range(half)], axis=1)
        for mine in range(2):
            left = jnp.concatenate(
                [
                    panel(recv_ab, p, left_chunk, 0) if mine else panel(recv_a, p, left_chunk)
                    for p in range(half)
                ],
                axis=1,
            )
            product = contract_first(left, right)
            base = (near if mine else 1 - near) * half
            for q in range(half):
                at = q * lanes
                for p in range(half):
                    piece = product[at : at + width, p * lanes : (p + 1) * lanes]
                    for k in range(1, own):
                        low = at + k * width
                        piece = jnp.where(
                            group == k,
                            product[low : low + width, p * lanes : (p + 1) * lanes],
                            piece,
                        )
                    send_own[chunk, p, (base + q) * CHUNKS + left_chunk] = piece.astype(BF16)

    for chunk in range(CHUNKS):
        wait_ab(recv_sem, chunk)
        if chunk < CHUNKS - 1:
            for other in range(chunk + 1):
                pieces(chunk, other)
                if other < chunk:
                    pieces(other, chunk)
    last = CHUNKS - 1
    for chunk in range(last):
        pieces(last, chunk)
        start_own(chunk)
    for other in range(CHUNKS):
        pieces(other, last)
    start_own(last)

    for chunk in range(CHUNKS):
        wait_own(recv_sem, chunk)
        final = back(1, chunk, recv_own[chunk].astype(F32))
        out_ref[:, chunk * width : (chunk + 1) * width, :] = (
            jnp.transpose(final).reshape(tile_rows, width, channels).astype(BF16)
        )
    for chunk in range(CHUNKS):
        wait_sum(send_sem, chunk)
        wait_ab(send_sem, chunk)
        wait_own(send_sem, chunk)
    wait_k(send_sem)


def fused(row_count, col_count, *args):
    tile_rows, tile_cols, channels = args[0].shape
    devices = row_count * col_count
    hidden = args[-1].shape[1]
    half = col_count // 2
    owners = row_count * half
    width = tile_cols // CHUNKS
    lanes = hidden // owners * width
    pairs = tile_rows * width
    vmem = pl.BlockSpec(memory_space=pltpu.VMEM)
    return pl.pallas_call(
        functools.partial(fused_kernel, row_count, col_count),
        out_shape=jax.ShapeDtypeStruct(args[0].shape, BF16),
        in_specs=[pl.BlockSpec(memory_space=pl.ANY)] * len(args),
        out_specs=vmem,
        scratch_shapes=[pltpu.VMEM(arg.shape, arg.dtype) for arg in args]
        + [
            pltpu.SemaphoreType.DMA((len(args),)),
            pltpu.VMEM((CHUNKS, channels, pairs), F32),
            pltpu.VMEM((2, tile_rows * owners, lanes), F32),
            pltpu.VMEM((CHUNKS, channels, pairs), F32),
            pltpu.VMEM((2, channels, lanes), F32),
            pltpu.VMEM((2, channels, lanes), F32),
            pltpu.VMEM((2, owners, lanes), F32),
            pltpu.VMEM((2, owners, lanes), F32),
            pltpu.VMEM((owners, CHUNKS, 2, tile_rows, lanes), BF16),
            pltpu.VMEM((owners, CHUNKS, 2, tile_rows, lanes), BF16),
            pltpu.VMEM((CHUNKS, owners, 2, tile_rows, lanes), BF16),
            pltpu.VMEM((CHUNKS, owners, tile_rows, lanes), BF16),
            pltpu.VMEM((CHUNKS, owners, 2, tile_rows, lanes), BF16),
            pltpu.VMEM((CHUNKS, col_count, row_count, tile_rows, lanes), BF16),
            pltpu.VMEM((CHUNKS, devices, tile_rows, lanes), BF16),
            pltpu.VMEM((CHUNKS, half, row_count, tile_rows, lanes), BF16),
            pltpu.VMEM((CHUNKS, owners, tile_rows, lanes), BF16),
            pltpu.SemaphoreType.DMA((5 * CHUNKS,)),
            pltpu.SemaphoreType.DMA((5 * CHUNKS,)),
        ],
        compiler_params=pltpu.CompilerParams(collective_id=0, has_side_effects=True),
    )(*args)


def solution(mesh):
    row_count, col_count = mesh.shape["row"], mesh.shape["col"]
    devices = row_count * col_count

    def step(*args):
        tile_rows, tile_cols, channels = args[0].shape
        hidden = args[-1].shape[1]
        owners = devices // 2
        own = hidden // owners
        width = tile_cols // CHUNKS
        fits = (
            hidden % devices == 0
            and col_count % 2 == 0
            and tile_cols % CHUNKS == 0
            and own * width == 128
            and tile_rows == width
            and tile_rows % 16 == 0
            and tile_rows % own == 0
            and own & (own - 1) == 0
            and row_count & (row_count - 1) == 0
            and col_count & (col_count - 1) == 0
            and row_count * tile_rows == col_count * tile_cols
        )
        return fused(row_count, col_count, *args) if fits else on_device(*args)

    return jax.shard_map(
        step,
        mesh=mesh,
        in_specs=(P("row", "col", None), P("row", "col"), P(), P(), P(), P(), P(), P(), P()),
        out_specs=P("row", "col", None),
        check_vma=False,
    )
```

```python
import functools

import jax
import jax.numpy as jnp
from jax import lax
from jax.experimental import pallas as pl
from jax.experimental.pallas import tpu as pltpu
from jax.sharding import PartitionSpec as P

epsilon = 1e-05


def normalize(values, weight_scale, weight_shift, reduce_axis):
    average = jnp.mean(values, axis=reduce_axis, keepdims=True)
    centred = values - average
    spread = jnp.mean(centred * centred, axis=reduce_axis, keepdims=True)
    return centred * lax.rsqrt(spread + epsilon) * weight_scale + weight_shift


def contract(left_panel, right_panel, layer_index):
    if layer_index == 0:
        product = jnp.einsum(
            "cik,cjk->cij", left_panel, right_panel, preferred_element_type=jnp.float32
        )
    else:
        product = jnp.einsum(
            "cki,ckj->cij", left_panel, right_panel, preferred_element_type=jnp.float32
        )
    return product.astype(jnp.bfloat16)


def gated_panel(pair_ln, weights, first, hidden, mask_float):
    projected = jnp.einsum(
        "ijd,de->eij",
        pair_ln,
        weights[:, first : first + 2 * hidden],
        preferred_element_type=jnp.float32,
    )
    return (jax.nn.sigmoid(projected[:hidden]) * projected[hidden:] * mask_float).astype(
        jnp.bfloat16
    )


def on_device(
    pair_state,
    pair_mask,
    input_gain,
    input_bias,
    proj_weights,
    gate_weights,
    output_gain,
    output_bias,
    output_weights,
):
    tile_rows, tile_cols, channels = pair_state.shape
    hidden = output_weights.shape[1]
    row_count = lax.axis_size("row")
    col_count = lax.axis_size("col")
    per_device = hidden // (row_count * col_count)
    current = pair_state.astype(jnp.float32)
    mask_float = pair_mask.astype(jnp.float32)[None]
    for layer_index in range(2):
        pair_ln = normalize(current, input_gain[layer_index], input_bias[layer_index], -1).astype(
            jnp.bfloat16
        )
        left_panel = gated_panel(pair_ln, proj_weights[layer_index], 0, hidden, mask_float)
        right_panel = gated_panel(
            pair_ln, proj_weights[layer_index], 2 * hidden, hidden, mask_float
        )
        gate_value = jax.nn.sigmoid(
            jnp.einsum(
                "ijd,de->ije",
                pair_ln,
                gate_weights[layer_index],
                preferred_element_type=jnp.float32,
            )
        )
        scale_out = output_gain[layer_index]
        shift_out = output_bias[layer_index]
        weight_out = output_weights[layer_index]
        left_recv, right_recv = (
            lax.all_to_all(left_panel, ("row", "col"), split_axis=0, concat_axis=1, tiled=True),
            lax.all_to_all(right_panel, ("row", "col"), split_axis=0, concat_axis=1, tiled=True),
        )
        left_chan = (
            left_recv.reshape(per_device, row_count, col_count, tile_rows, tile_cols)
            .transpose(0, 1, 3, 2, 4)
            .reshape(per_device, row_count * tile_rows, col_count * tile_cols)
        )
        right_chan = (
            right_recv.reshape(per_device, row_count, col_count, tile_rows, tile_cols)
            .transpose(0, 1, 3, 2, 4)
            .reshape(per_device, row_count * tile_rows, col_count * tile_cols)
        )
        product = contract(left_chan, right_chan, layer_index)
        arranged = (
            product.reshape(per_device, row_count, tile_rows, col_count, tile_cols)
            .transpose(0, 1, 3, 2, 4)
            .reshape(per_device, row_count * col_count * tile_rows, tile_cols)
        )
        returned = lax.all_to_all(arranged, ("row", "col"), split_axis=1, concat_axis=0, tiled=True)
        normed = normalize(
            returned.astype(jnp.float32), scale_out[:, None, None], shift_out[:, None, None], 0
        ).astype(jnp.bfloat16)
        update = jnp.einsum("cij,cd->ijd", normed, weight_out, preferred_element_type=jnp.float32)
        current = current + gate_value * update
    return current.astype(jnp.bfloat16)


MESH = pl.DeviceIdType.MESH
F32 = jnp.float32
BF16 = jnp.bfloat16
CHUNKS = 2


def sigmoid(values):
    return 0.5 * jnp.tanh(0.5 * values) + 0.5


def lane_groups(shape, width):
    return lax.broadcasted_iota(jnp.int32, shape, len(shape) - 1) // width


def swap_groups(blocks, width):
    count = len(blocks)
    blocks = list(blocks)
    lanes = count * width
    group = lane_groups(blocks[0].shape, width)
    step = count // 2
    while step:
        low = (group // step) % 2 == 0
        for p in range(count):
            if p & step:
                continue
            first, second = blocks[p], blocks[p + step]
            shift = step * width
            blocks[p] = jnp.where(low, first, pltpu.roll(second, shift, 1))
            blocks[p + step] = jnp.where(low, pltpu.roll(first, lanes - shift, 1), second)
        step //= 2
    return blocks


def columns_of(row_vector, lanes):
    return jnp.transpose(jnp.broadcast_to(row_vector, (lanes, row_vector.shape[1])))


def contract_first(left, right):
    return lax.dot_general(left, right, (((0,), (0,)), ((), ())), preferred_element_type=F32)


def fused_kernel(row_count, col_count, *refs):
    operands, out_ref, held = refs[:9], refs[9], refs[10:19]
    load_sem = refs[19]
    loads = [
        pltpu.make_async_copy(source, target, load_sem.at[at])
        for at, (source, target) in enumerate(zip(operands, held))
    ]
    for at in (0, 4, 2, 3, 1, 5, 6, 7, 8):
        loads[at].start()
    fused_body(row_count, col_count, loads, *held, out_ref, *refs[20:])


def fused_body(
    row_count,
    col_count,
    loads,
    z_ref,
    mask_ref,
    in_gain,
    in_bias,
    proj_ref,
    gate_ref,
    out_gain,
    out_bias,
    outw_ref,
    out_ref,
    zt_ref,
    tmp_ref,
    gated_ref,
    projt_ref,
    outwt_ref,
    in_gain_ref,
    in_bias_ref,
    gain_ref,
    bias_ref,
    send_k,
    recv_k,
    send_ab,
    recv_a,
    recv_ab,
    send_sum,
    recv_sum,
    send_own,
    recv_own,
    send_sem,
    recv_sem,
):
    tile_rows, tile_cols, channels = z_ref.shape
    devices = row_count * col_count
    hidden = outw_ref.shape[1]
    half = col_count // 2
    width = tile_cols // CHUNKS
    pairs = tile_rows * width
    owners = row_count * half
    own = hidden // owners
    lanes = own * width
    blocks = pairs // lanes
    tokens = row_count * tile_rows
    row, col = lax.axis_index("row"), lax.axis_index("col")
    near, inner = col // half, lax.rem(col, half)
    me = row * half + inner

    def flips(index, count):
        bits = count.bit_length() - 1
        moves = [(1 << b) * (1 - 2 * lax.rem(index // (1 << b), 2)) for b in range(bits)]

        def flipped(pattern):
            total = index
            for b in range(bits):
                if pattern >> b & 1:
                    total = total + moves[b]
            return total

        return [flipped(pattern) for pattern in range(count)]

    rows, cols = flips(row, row_count), flips(col, col_count)
    row_order = sorted(range(row_count), key=lambda p: (-p.bit_count(), -p))
    across = list(range(half, col_count))
    within = list(range(half - 1, -1, -1))

    def each(action, turns):
        for turn in turns:
            for step in row_order:
                if turn or step:
                    action(rows[step], cols[turn])

    barrier = pltpu.get_barrier_semaphore()

    def greet(trow, tcol):
        pl.semaphore_signal(barrier, inc=1, device_id=(trow, tcol), device_id_type=MESH)

    greet(row, cols[half])
    each(greet, within)

    def send(source, target, at, trow, tcol):
        pltpu.make_async_remote_copy(
            src_ref=source,
            dst_ref=target,
            send_sem=send_sem.at[at],
            recv_sem=recv_sem.at[at],
            device_id=(trow, tcol),
            device_id_type=MESH,
        ).start()

    def owner(trow, tcol):
        return trow * half + lax.rem(tcol, half)

    slot = inner * row_count + row

    def start_k():
        each(
            lambda trow, tcol: send(send_k.at[owner(trow, tcol)], recv_k.at[slot], 0, trow, tcol),
            within,
        )
        recv_k[slot] = send_k[me]

    def wait_k(sem):
        slots = recv_k.at[pl.ds(0, owners - 1)]
        pltpu.make_async_copy(slots, slots, sem.at[0]).wait()

    def start_sum(chunk):
        each(
            lambda trow, tcol: send(
                send_sum.at[chunk, tcol, trow],
                recv_sum.at[chunk, near * owners + me],
                CHUNKS + chunk,
                trow,
                tcol,
            ),
            across + within,
        )
        recv_sum[chunk, near * owners + me] = send_sum[chunk, col, row]

    def wait_sum(sem, chunk):
        slots = recv_sum.at[chunk, pl.ds(0, devices - 1)]
        pltpu.make_async_copy(slots, slots, sem.at[CHUNKS + chunk]).wait()

    def start_a(chunk):
        each(
            lambda trow, tcol: send(
                send_ab.at[chunk, owner(trow, tcol), 0],
                recv_a.at[chunk, slot],
                2 * CHUNKS + chunk,
                trow,
                tcol,
            ),
            across,
        )

    def start_ab(chunk):
        each(
            lambda trow, tcol: send(
                send_ab.at[chunk, owner(trow, tcol)],
                recv_ab.at[chunk, slot],
                3 * CHUNKS + chunk,
                trow,
                tcol,
            ),
            within,
        )
        recv_ab[chunk, slot] = send_ab[chunk, me]

    def wait_ab(sem, chunk):
        slots = recv_a.at[chunk]
        pltpu.make_async_copy(slots, slots, sem.at[2 * CHUNKS + chunk]).wait()
        slots = recv_ab.at[chunk, pl.ds(0, owners - 1)]
        pltpu.make_async_copy(slots, slots, sem.at[3 * CHUNKS + chunk]).wait()

    def start_own(chunk):
        each(
            lambda trow, tcol: send(
                send_own.at[chunk, lax.rem(tcol, half), trow],
                recv_own.at[chunk, me],
                4 * CHUNKS + chunk,
                trow,
                tcol,
            ),
            within,
        )
        recv_own[chunk, me] = send_own[chunk, inner, row]

    def wait_own(sem, chunk):
        slots = recv_own.at[chunk, pl.ds(0, owners - 1)]
        pltpu.make_async_copy(slots, slots, sem.at[4 * CHUNKS + chunk]).wait()

    def spread_inputs(layer):
        in_gain_ref[layer] = columns_of(in_gain[layer : layer + 1, :], lanes)
        in_bias_ref[layer] = columns_of(in_bias[layer : layer + 1, :], lanes)

    def spread_outputs(layer):
        group = lane_groups((owners, lanes), width)
        for source, kept in ((out_gain, gain_ref), (out_bias, bias_ref)):
            wide = columns_of(source[layer : layer + 1, :], lanes)
            packed = wide[0:owners]
            for k in range(1, own):
                packed = jnp.where(group == k, wide[k * owners : (k + 1) * owners], packed)
            kept[layer] = packed

    def front(layer, current, mask_flat, target_at, sent=None):
        centred = current - jnp.mean(current, axis=0, keepdims=True)
        scale = lax.rsqrt(jnp.mean(centred * centred, axis=0, keepdims=True) + epsilon)
        gain = jnp.concatenate([in_gain_ref[layer]] * blocks, axis=1)
        bias = jnp.concatenate([in_bias_ref[layer]] * blocks, axis=1)
        normed = (centred * scale * gain + bias).astype(BF16)
        for side in range(2):
            first = 2 * side * hidden
            if layer == 0:
                weights = proj_ref[layer, :, first : first + 2 * hidden]
                projected = contract_first(weights, normed)
            else:
                weights = projt_ref[first : first + 2 * hidden]
                projected = jnp.dot(weights, normed, preferred_element_type=F32)
            panel = sigmoid(projected[:hidden]) * projected[hidden:] * mask_flat
            for block in range(blocks):
                parts = [
                    panel[k * owners : (k + 1) * owners, block * lanes : (block + 1) * lanes]
                    for k in range(own)
                ]
                for q, part in enumerate(swap_groups(parts, width)):
                    line = block * own + q
                    tmp_ref[side, line * owners : (line + 1) * owners, :] = part
            for target in range(owners):
                target_at(target)[side] = tmp_ref[
                    side, pl.ds(target, tile_rows, stride=owners), :
                ].astype(BF16)
            if sent is not None:
                sent[side]()
        return normed

    def gate(layer, chunk, normed):
        gated_ref[chunk] = sigmoid(contract_first(gate_ref[layer], normed))

    def over_channels(values):
        total = jnp.sum(values, axis=0)
        shift = lanes // 2
        while shift >= width:
            total = total + pltpu.roll(total, shift, 1)
            shift //= 2
        return total * (1.0 / hidden)

    def back(layer, chunk, returned):
        centred = returned - over_channels(returned)[None]
        scale = lax.rsqrt(over_channels(centred * centred) + epsilon)
        for d in range(owners):
            tmp_ref[0, d * tile_rows : (d + 1) * tile_rows, :] = (
                centred[d] * scale * gain_ref[layer, d : d + 1, :] + bias_ref[layer, d : d + 1, :]
            )
        wide_blocks = []
        for block in range(blocks):
            parts = [
                tmp_ref[0, pl.ds(block * own + q, owners, stride=tile_rows), :] for q in range(own)
            ]
            wide_blocks.append(jnp.concatenate(swap_groups(parts, width), axis=0).astype(BF16))
        update = jnp.dot(
            outwt_ref[layer], jnp.concatenate(wide_blocks, axis=1), preferred_element_type=F32
        )
        return zt_ref[chunk] + gated_ref[chunk] * update

    for at in (2, 3):
        loads[at].wait()
    spread_inputs(0)
    loads[1].wait()
    mask_float = mask_ref[...].astype(F32)
    column = lax.broadcasted_iota(jnp.int32, (tile_cols, pairs), 1) % width
    mine = (
        lax.broadcasted_iota(jnp.int32, (tile_rows, pairs), 1) // width
        == lax.broadcasted_iota(jnp.int32, (tile_rows, pairs), 0)
    ).astype(F32)
    mask_flat = []
    for chunk in range(CHUNKS):
        spread = (
            column + chunk * width == lax.broadcasted_iota(jnp.int32, (tile_cols, pairs), 0)
        ).astype(F32)
        mask_flat.append(
            jnp.sum(
                jnp.dot(mask_float, spread, preferred_element_type=F32) * mine,
                axis=0,
                keepdims=True,
            )
        )
    loads[0].wait()
    loads[4].wait()
    normed = [None] * CHUNKS
    for chunk in range(CHUNKS):
        zt_ref[chunk] = jnp.transpose(
            z_ref[:, chunk * width : (chunk + 1) * width, :].astype(F32).reshape(pairs, channels)
        )
        normed[chunk] = front(
            0,
            zt_ref[chunk],
            mask_flat[chunk],
            lambda target, chunk=chunk: send_k.at[target, chunk],
        )
    pl.semaphore_wait(barrier, owners)
    start_k()
    for at in (5, 6, 7, 8):
        loads[at].wait()
    for layer in range(1, 2):
        projt_ref[...] = jnp.transpose(proj_ref[layer])
    for layer in range(2):
        outwt_ref[layer] = jnp.transpose(outw_ref[layer])
    for chunk in range(CHUNKS):
        gate(0, chunk, normed[chunk])
    spread_inputs(1)
    for layer in range(2):
        spread_outputs(layer)
    wait_k(recv_sem)

    def panel(ref, plane, *at):
        span = (slice(plane * row_count, (plane + 1) * row_count),)
        return ref[at[:1] + span + at[1:] if ref is not recv_k else span + at].reshape(tokens, lanes)

    spans = [(chunk, plane) for chunk in range(CHUNKS) for plane in range(half)]
    left = jnp.concatenate([panel(recv_k, p, c, 0) for c, p in spans], axis=1)
    right = jnp.concatenate([panel(recv_k, p, c, 1) for c, p in spans], axis=1)
    lane_group = lane_groups((1, len(spans) * lanes), width) % own
    masks = [(lane_group == k).astype(F32).astype(BF16) for k in range(own)]
    for chunk in range(CHUNKS):
        for c in range(col_count):
            at = (c * CHUNKS + chunk) * width
            lines = right[at : at + width]
            stacked = jnp.concatenate([lines * masks[k] for k in range(own)], axis=0)
            product = lax.dot_general(
                left, stacked, (((1,), (1,)), ((), ())), preferred_element_type=F32
            )
            send_sum[chunk, c] = product.astype(BF16).reshape(row_count, tile_rows, lanes)
        start_sum(chunk)

    for chunk in range(CHUNKS):
        wait_sum(recv_sem, chunk)
        returned = recv_sum[chunk, 0:owners].astype(F32) + recv_sum[
            chunk, owners : 2 * owners
        ].astype(F32)
        zt_ref[chunk] = back(0, chunk, returned)
        normed[chunk] = front(
            1,
            zt_ref[chunk],
            mask_flat[chunk],
            lambda target, chunk=chunk: send_ab.at[chunk, target],
            (lambda chunk=chunk: start_a(chunk), lambda chunk=chunk: start_ab(chunk)),
        )
    for chunk in range(CHUNKS):
        gate(1, chunk, normed[chunk])
    group = lane_groups((width, lanes), width)

    def pieces(left_chunk, chunk):
        right = jnp.concatenate([panel(recv_ab, p, chunk, 1) for p in range(half)], axis=1)
        for mine in range(2):
            left = jnp.concatenate(
                [
                    panel(recv_ab, p, left_chunk, 0) if mine else panel(recv_a, p, left_chunk)
                    for p in range(half)
                ],
                axis=1,
            )
            product = contract_first(left, right)
            base = (near if mine else 1 - near) * half
            for q in range(half):
                at = q * lanes
                for p in range(half):
                    piece = product[at : at + width, p * lanes : (p + 1) * lanes]
                    for k in range(1, own):
                        low = at + k * width
                        piece = jnp.where(
                            group == k,
                            product[low : low + width, p * lanes : (p + 1) * lanes],
                            piece,
                        )
                    send_own[chunk, p, (base + q) * CHUNKS + left_chunk] = piece.astype(BF16)

    for chunk in range(CHUNKS):
        wait_ab(recv_sem, chunk)
        if chunk < CHUNKS - 1:
            for other in range(chunk + 1):
                pieces(chunk, other)
                if other < chunk:
                    pieces(other, chunk)
    last = CHUNKS - 1
    for chunk in range(last):
        pieces(last, chunk)
        start_own(chunk)
    for other in range(CHUNKS):
        pieces(other, last)
    start_own(last)

    for chunk in range(CHUNKS):
        wait_own(recv_sem, chunk)
        final = back(1, chunk, recv_own[chunk].astype(F32))
        out_ref[:, chunk * width : (chunk + 1) * width, :] = (
            jnp.transpose(final).reshape(tile_rows, width, channels).astype(BF16)
        )
    for chunk in range(CHUNKS):
        wait_sum(send_sem, chunk)
        wait_ab(send_sem, chunk)
        wait_own(send_sem, chunk)
    wait_k(send_sem)


def fused(row_count, col_count, *args):
    tile_rows, tile_cols, channels = args[0].shape
    devices = row_count * col_count
    hidden = args[-1].shape[1]
    half = col_count // 2
    owners = row_count * half
    width = tile_cols // CHUNKS
    lanes = hidden // owners * width
    pairs = tile_rows * width
    vmem = pl.BlockSpec(memory_space=pltpu.VMEM)
    return pl.pallas_call(
        functools.partial(fused_kernel, row_count, col_count),
        out_shape=jax.ShapeDtypeStruct(args[0].shape, BF16),
        in_specs=[pl.BlockSpec(memory_space=pl.ANY)] * len(args),
        out_specs=vmem,
        scratch_shapes=[pltpu.VMEM(arg.shape, arg.dtype) for arg in args]
        + [
            pltpu.SemaphoreType.DMA((len(args),)),
            pltpu.VMEM((CHUNKS, channels, pairs), F32),
            pltpu.VMEM((2, tile_rows * owners, lanes), F32),
            pltpu.VMEM((CHUNKS, channels, pairs), F32),
            pltpu.VMEM(args[4].shape[:0:-1], BF16),
            pltpu.VMEM(args[8].shape[:1] + args[8].shape[:0:-1], BF16),
            pltpu.VMEM((2, channels, lanes), F32),
            pltpu.VMEM((2, channels, lanes), F32),
            pltpu.VMEM((2, owners, lanes), F32),
            pltpu.VMEM((2, owners, lanes), F32),
            pltpu.VMEM((owners, CHUNKS, 2, tile_rows, lanes), BF16),
            pltpu.VMEM((owners, CHUNKS, 2, tile_rows, lanes), BF16),
            pltpu.VMEM((CHUNKS, owners, 2, tile_rows, lanes), BF16),
            pltpu.VMEM((CHUNKS, owners, tile_rows, lanes), BF16),
            pltpu.VMEM((CHUNKS, owners, 2, tile_rows, lanes), BF16),
            pltpu.VMEM((CHUNKS, col_count, row_count, tile_rows, lanes), BF16),
            pltpu.VMEM((CHUNKS, devices, tile_rows, lanes), BF16),
            pltpu.VMEM((CHUNKS, half, row_count, tile_rows, lanes), BF16),
            pltpu.VMEM((CHUNKS, owners, tile_rows, lanes), BF16),
            pltpu.SemaphoreType.DMA((5 * CHUNKS,)),
            pltpu.SemaphoreType.DMA((5 * CHUNKS,)),
        ],
        compiler_params=pltpu.CompilerParams(
            collective_id=0, has_side_effects=True, vmem_limit_bytes=16 << 20
        ),
    )(*[pltpu.with_memory_space_constraint(arg, pltpu.HBM) for arg in args])


def solution(mesh):
    row_count, col_count = mesh.shape["row"], mesh.shape["col"]
    devices = row_count * col_count

    def step(*args):
        tile_rows, tile_cols, channels = args[0].shape
        hidden = args[-1].shape[1]
        owners = devices // 2
        own = hidden // owners
        width = tile_cols // CHUNKS
        fits = (
            hidden % devices == 0
            and col_count % 2 == 0
            and tile_cols % CHUNKS == 0
            and own * width == 128
            and tile_rows == width
            and tile_rows % 16 == 0
            and tile_rows % own == 0
            and own & (own - 1) == 0
            and row_count & (row_count - 1) == 0
            and col_count & (col_count - 1) == 0
            and row_count * tile_rows == col_count * tile_cols
        )
        return fused(row_count, col_count, *args) if fits else on_device(*args)

    return jax.shard_map(
        step,
        mesh=mesh,
        in_specs=(P("row", "col", None), P("row", "col"), P(), P(), P(), P(), P(), P(), P()),
        out_specs=P("row", "col", None),
        check_vma=False,
    )
```

```python
import functools

import jax
import jax.numpy as jnp
from jax import lax
from jax.experimental import pallas as pl
from jax.experimental.pallas import tpu as pltpu
from jax.sharding import PartitionSpec as P

epsilon = 1e-05


def normalize(values, weight_scale, weight_shift, reduce_axis):
    average = jnp.mean(values, axis=reduce_axis, keepdims=True)
    centred = values - average
    spread = jnp.mean(centred * centred, axis=reduce_axis, keepdims=True)
    return centred * lax.rsqrt(spread + epsilon) * weight_scale + weight_shift


def contract(left_panel, right_panel, layer_index):
    if layer_index == 0:
        product = jnp.einsum(
            "cik,cjk->cij", left_panel, right_panel, preferred_element_type=jnp.float32
        )
    else:
        product = jnp.einsum(
            "cki,ckj->cij", left_panel, right_panel, preferred_element_type=jnp.float32
        )
    return product.astype(jnp.bfloat16)


def gated_panel(pair_ln, weights, first, hidden, mask_float):
    projected = jnp.einsum(
        "ijd,de->eij",
        pair_ln,
        weights[:, first : first + 2 * hidden],
        preferred_element_type=jnp.float32,
    )
    return (jax.nn.sigmoid(projected[:hidden]) * projected[hidden:] * mask_float).astype(
        jnp.bfloat16
    )


def on_device(
    pair_state,
    pair_mask,
    input_gain,
    input_bias,
    proj_weights,
    gate_weights,
    output_gain,
    output_bias,
    output_weights,
):
    tile_rows, tile_cols, channels = pair_state.shape
    hidden = output_weights.shape[1]
    row_count = lax.axis_size("row")
    col_count = lax.axis_size("col")
    per_device = hidden // (row_count * col_count)
    current = pair_state.astype(jnp.float32)
    mask_float = pair_mask.astype(jnp.float32)[None]
    for layer_index in range(2):
        pair_ln = normalize(current, input_gain[layer_index], input_bias[layer_index], -1).astype(
            jnp.bfloat16
        )
        left_panel = gated_panel(pair_ln, proj_weights[layer_index], 0, hidden, mask_float)
        right_panel = gated_panel(
            pair_ln, proj_weights[layer_index], 2 * hidden, hidden, mask_float
        )
        gate_value = jax.nn.sigmoid(
            jnp.einsum(
                "ijd,de->ije",
                pair_ln,
                gate_weights[layer_index],
                preferred_element_type=jnp.float32,
            )
        )
        scale_out = output_gain[layer_index]
        shift_out = output_bias[layer_index]
        weight_out = output_weights[layer_index]
        left_recv, right_recv = (
            lax.all_to_all(left_panel, ("row", "col"), split_axis=0, concat_axis=1, tiled=True),
            lax.all_to_all(right_panel, ("row", "col"), split_axis=0, concat_axis=1, tiled=True),
        )
        left_chan = (
            left_recv.reshape(per_device, row_count, col_count, tile_rows, tile_cols)
            .transpose(0, 1, 3, 2, 4)
            .reshape(per_device, row_count * tile_rows, col_count * tile_cols)
        )
        right_chan = (
            right_recv.reshape(per_device, row_count, col_count, tile_rows, tile_cols)
            .transpose(0, 1, 3, 2, 4)
            .reshape(per_device, row_count * tile_rows, col_count * tile_cols)
        )
        product = contract(left_chan, right_chan, layer_index)
        arranged = (
            product.reshape(per_device, row_count, tile_rows, col_count, tile_cols)
            .transpose(0, 1, 3, 2, 4)
            .reshape(per_device, row_count * col_count * tile_rows, tile_cols)
        )
        returned = lax.all_to_all(arranged, ("row", "col"), split_axis=1, concat_axis=0, tiled=True)
        normed = normalize(
            returned.astype(jnp.float32), scale_out[:, None, None], shift_out[:, None, None], 0
        ).astype(jnp.bfloat16)
        update = jnp.einsum("cij,cd->ijd", normed, weight_out, preferred_element_type=jnp.float32)
        current = current + gate_value * update
    return current.astype(jnp.bfloat16)


MESH = pl.DeviceIdType.MESH
F32 = jnp.float32
BF16 = jnp.bfloat16
CHUNKS = 2


def sigmoid(values):
    return 0.5 * jnp.tanh(0.5 * values) + 0.5


def lane_groups(shape, width):
    return lax.broadcasted_iota(jnp.int32, shape, len(shape) - 1) // width


def swap_groups(blocks, width):
    count = len(blocks)
    lanes = count * width
    group = lane_groups(blocks[0].shape, width)
    held = [pltpu.roll(part, at * width, 1) if at else part for at, part in enumerate(blocks)]
    step = 1
    while step < count:
        high = (group // step) % 2 == 1
        held = [jnp.where(high, held[(at + step) % count], held[at]) for at in range(count)]
        step *= 2
    return [
        pltpu.roll(held[-at % count], lanes - at * width, 1) if at else held[0]
        for at in range(count)
    ]


def columns_of(row_vector, lanes):
    return jnp.transpose(jnp.broadcast_to(row_vector, (lanes, row_vector.shape[1])))


def contract_first(left, right):
    return lax.dot_general(left, right, (((0,), (0,)), ((), ())), preferred_element_type=F32)


def fused_kernel(row_count, col_count, *refs):
    operands, out_ref, held = refs[:9], refs[9], refs[10:19]
    load_sem = refs[19]
    loads = [
        pltpu.make_async_copy(source, target, load_sem.at[at])
        for at, (source, target) in enumerate(zip(operands, held))
    ]
    for at in (0, 4, 2, 3, 1, 5, 6, 7, 8):
        loads[at].start()
    fused_body(row_count, col_count, loads, *held, out_ref, *refs[20:])


def fused_body(
    row_count,
    col_count,
    loads,
    z_ref,
    mask_ref,
    in_gain,
    in_bias,
    proj_ref,
    gate_ref,
    out_gain,
    out_bias,
    outw_ref,
    out_ref,
    zt_ref,
    tmp_ref,
    gated_ref,
    projt_ref,
    outwt_ref,
    in_gain_ref,
    in_bias_ref,
    gain_ref,
    bias_ref,
    send_k,
    recv_k,
    send_ab,
    recv_a,
    recv_ab,
    send_sum,
    recv_sum,
    send_own,
    recv_own,
    send_sem,
    recv_sem,
):
    tile_rows, tile_cols, channels = z_ref.shape
    devices = row_count * col_count
    hidden = outw_ref.shape[1]
    half = col_count // 2
    width = tile_cols // CHUNKS
    pairs = tile_rows * width
    owners = row_count * half
    own = hidden // owners
    lanes = own * width
    blocks = pairs // lanes
    tokens = row_count * tile_rows
    row, col = lax.axis_index("row"), lax.axis_index("col")
    near, inner = col // half, lax.rem(col, half)
    me = row * half + inner

    def flips(index, count):
        bits = count.bit_length() - 1
        moves = [(1 << b) * (1 - 2 * lax.rem(index // (1 << b), 2)) for b in range(bits)]

        def flipped(pattern):
            total = index
            for b in range(bits):
                if pattern >> b & 1:
                    total = total + moves[b]
            return total

        return [flipped(pattern) for pattern in range(count)]

    rows, cols = flips(row, row_count), flips(col, col_count)
    row_order = sorted(range(row_count), key=lambda p: (-p.bit_count(), -p))
    across = list(range(half, col_count))
    within = list(range(half - 1, -1, -1))

    def each(action, turns):
        for turn in turns:
            for step in row_order:
                if turn or step:
                    action(rows[step], cols[turn])

    barrier = pltpu.get_barrier_semaphore()

    def greet(trow, tcol):
        pl.semaphore_signal(barrier, inc=1, device_id=(trow, tcol), device_id_type=MESH)

    greet(row, cols[half])
    each(greet, within)

    def send(source, target, at, trow, tcol):
        pltpu.make_async_remote_copy(
            src_ref=source,
            dst_ref=target,
            send_sem=send_sem.at[at],
            recv_sem=recv_sem.at[at],
            device_id=(trow, tcol),
            device_id_type=MESH,
        ).start()

    def owner(trow, tcol):
        return trow * half + lax.rem(tcol, half)

    slot = inner * row_count + row

    def start_k():
        each(
            lambda trow, tcol: send(send_k.at[owner(trow, tcol)], recv_k.at[slot], 0, trow, tcol),
            within,
        )
        recv_k[slot] = send_k[me]

    def wait_k(sem):
        slots = recv_k.at[pl.ds(0, owners - 1)]
        pltpu.make_async_copy(slots, slots, sem.at[0]).wait()

    def start_sum(chunk):
        each(
            lambda trow, tcol: send(
                send_sum.at[chunk, tcol, trow],
                recv_sum.at[chunk, near * owners + me],
                CHUNKS + chunk,
                trow,
                tcol,
            ),
            across + within,
        )
        recv_sum[chunk, near * owners + me] = send_sum[chunk, col, row]

    def wait_sum(sem, chunk):
        slots = recv_sum.at[chunk, pl.ds(0, devices - 1)]
        pltpu.make_async_copy(slots, slots, sem.at[CHUNKS + chunk]).wait()

    def start_a(chunk):
        each(
            lambda trow, tcol: send(
                send_ab.at[chunk, owner(trow, tcol), 0],
                recv_a.at[chunk, slot],
                2 * CHUNKS + chunk,
                trow,
                tcol,
            ),
            across,
        )

    def start_ab(chunk):
        each(
            lambda trow, tcol: send(
                send_ab.at[chunk, owner(trow, tcol)],
                recv_ab.at[chunk, slot],
                3 * CHUNKS + chunk,
                trow,
                tcol,
            ),
            within,
        )
        recv_ab[chunk, slot] = send_ab[chunk, me]

    def wait_ab(sem, chunk):
        slots = recv_a.at[chunk]
        pltpu.make_async_copy(slots, slots, sem.at[2 * CHUNKS + chunk]).wait()
        slots = recv_ab.at[chunk, pl.ds(0, owners - 1)]
        pltpu.make_async_copy(slots, slots, sem.at[3 * CHUNKS + chunk]).wait()

    def start_own():
        each(
            lambda trow, tcol: send(
                send_own.at[lax.rem(tcol, half), trow], recv_own.at[me], 4 * CHUNKS, trow, tcol
            ),
            within,
        )
        recv_own[me] = send_own[inner, row]

    def wait_own(sem):
        slots = recv_own.at[pl.ds(0, owners - 1)]
        pltpu.make_async_copy(slots, slots, sem.at[4 * CHUNKS]).wait()

    def spread_inputs(layer):
        in_gain_ref[layer] = columns_of(in_gain[layer : layer + 1, :], lanes)
        in_bias_ref[layer] = columns_of(in_bias[layer : layer + 1, :], lanes)

    def spread_outputs(layer):
        group = lane_groups((owners, lanes), width)
        for source, kept in ((out_gain, gain_ref), (out_bias, bias_ref)):
            wide = columns_of(source[layer : layer + 1, :], lanes)
            packed = wide[0:owners]
            for k in range(1, own):
                packed = jnp.where(group == k, wide[k * owners : (k + 1) * owners], packed)
            kept[layer] = packed

    def front(layer, current, mask_flat, target_at, sent=None):
        centred = current - jnp.mean(current, axis=0, keepdims=True)
        scale = lax.rsqrt(jnp.mean(centred * centred, axis=0, keepdims=True) + epsilon)
        gain = jnp.concatenate([in_gain_ref[layer]] * blocks, axis=1)
        bias = jnp.concatenate([in_bias_ref[layer]] * blocks, axis=1)
        normed = (centred * scale * gain + bias).astype(BF16)
        for side in range(2):
            first = 2 * side * hidden
            if layer == 0:
                weights = proj_ref[layer, :, first : first + 2 * hidden]
                projected = contract_first(weights, normed)
            else:
                weights = projt_ref[first : first + 2 * hidden]
                projected = jnp.dot(weights, normed, preferred_element_type=F32)
            panel = (sigmoid(projected[:hidden]) * projected[hidden:] * mask_flat).astype(BF16)
            for block in range(blocks):
                parts = [
                    panel[k * owners : (k + 1) * owners, block * lanes : (block + 1) * lanes]
                    for k in range(own)
                ]
                for q, part in enumerate(swap_groups(parts, width)):
                    line = block * own + q
                    tmp_ref[side, line * owners : (line + 1) * owners, :] = part.astype(F32)
            for target in range(owners):
                target_at(target)[side] = tmp_ref[
                    side, pl.ds(target, tile_rows, stride=owners), :
                ].astype(BF16)
            if sent is not None:
                sent[side]()
        return normed

    def gate(layer, chunk, normed):
        gated_ref[chunk] = sigmoid(contract_first(gate_ref[layer], normed))

    def over_channels(values):
        total = jnp.sum(values, axis=0)
        shift = lanes // 2
        while shift >= width:
            total = total + pltpu.roll(total, shift, 1)
            shift //= 2
        return total * (1.0 / hidden)

    def back(layer, chunk, returned):
        centred = returned - over_channels(returned)[None]
        scale = lax.rsqrt(over_channels(centred * centred) + epsilon)
        for d in range(owners):
            tmp_ref[chunk, d * tile_rows : (d + 1) * tile_rows, :] = (
                centred[d] * scale * gain_ref[layer, d : d + 1, :] + bias_ref[layer, d : d + 1, :]
            )
        wide_blocks = []
        for block in range(blocks):
            parts = [
                tmp_ref[chunk, pl.ds(block * own + q, owners, stride=tile_rows), :] for q in range(own)
            ]
            wide_blocks.append(jnp.concatenate(swap_groups(parts, width), axis=0).astype(BF16))
        update = jnp.dot(
            outwt_ref[layer], jnp.concatenate(wide_blocks, axis=1), preferred_element_type=F32
        )
        return zt_ref[chunk] + gated_ref[chunk] * update

    for at in (2, 3):
        loads[at].wait()
    spread_inputs(0)
    loads[1].wait()
    mask_float = mask_ref[...].astype(F32)
    column = lax.broadcasted_iota(jnp.int32, (tile_cols, pairs), 1) % width
    mine = (
        lax.broadcasted_iota(jnp.int32, (tile_rows, pairs), 1) // width
        == lax.broadcasted_iota(jnp.int32, (tile_rows, pairs), 0)
    ).astype(F32)
    mask_flat = []
    for chunk in range(CHUNKS):
        spread = (
            column + chunk * width == lax.broadcasted_iota(jnp.int32, (tile_cols, pairs), 0)
        ).astype(F32)
        mask_flat.append(
            jnp.sum(
                jnp.dot(mask_float, spread, preferred_element_type=F32) * mine,
                axis=0,
                keepdims=True,
            )
        )
    loads[0].wait()
    loads[4].wait()
    normed = [None] * CHUNKS
    for chunk in range(CHUNKS):
        zt_ref[chunk] = jnp.transpose(
            z_ref[:, chunk * width : (chunk + 1) * width, :].astype(F32).reshape(pairs, channels)
        )
        normed[chunk] = front(
            0,
            zt_ref[chunk],
            mask_flat[chunk],
            lambda target, chunk=chunk: send_k.at[target, chunk],
        )
    pl.semaphore_wait(barrier, owners)
    start_k()
    for at in (5, 6, 7, 8):
        loads[at].wait()
    for layer in range(1, 2):
        projt_ref[...] = jnp.transpose(proj_ref[layer])
    for layer in range(2):
        outwt_ref[layer] = jnp.transpose(outw_ref[layer])
    for chunk in range(CHUNKS):
        gate(0, chunk, normed[chunk])
    spread_inputs(1)
    for layer in range(2):
        spread_outputs(layer)
    wait_k(recv_sem)

    def panel(ref, plane, *at):
        span = (slice(plane * row_count, (plane + 1) * row_count),)
        return ref[at[:1] + span + at[1:] if ref is not recv_k else span + at].reshape(tokens, lanes)

    spans = [(chunk, plane) for chunk in range(CHUNKS) for plane in range(half)]
    left = jnp.concatenate([panel(recv_k, p, c, 0) for c, p in spans], axis=1)
    right = jnp.concatenate([panel(recv_k, p, c, 1) for c, p in spans], axis=1)
    lane_group = lane_groups((1, len(spans) * lanes), width) % own
    masks = [(lane_group == k).astype(F32).astype(BF16) for k in range(own)]
    for chunk in range(CHUNKS):
        for c in range(col_count):
            at = (c * CHUNKS + chunk) * width
            lines = right[at : at + width]
            stacked = jnp.concatenate([lines * masks[k] for k in range(own)], axis=0)
            product = lax.dot_general(
                left, stacked, (((1,), (1,)), ((), ())), preferred_element_type=F32
            )
            send_sum[chunk, c] = product.astype(BF16).reshape(row_count, tile_rows, lanes)
        start_sum(chunk)

    for chunk in range(CHUNKS):
        wait_sum(recv_sem, chunk)
        returned = recv_sum[chunk, 0:owners].astype(F32) + recv_sum[
            chunk, owners : 2 * owners
        ].astype(F32)
        zt_ref[chunk] = back(0, chunk, returned)
        normed[chunk] = front(
            1,
            zt_ref[chunk],
            mask_flat[chunk],
            lambda target, chunk=chunk: send_ab.at[chunk, target],
            (lambda chunk=chunk: start_a(chunk), lambda chunk=chunk: start_ab(chunk)),
        )
    for chunk in range(CHUNKS):
        gate(1, chunk, normed[chunk])
    group = lane_groups((width, lanes), width)

    def pieces(left_chunk, chunk):
        right = jnp.concatenate([panel(recv_ab, p, chunk, 1) for p in range(half)], axis=1)
        for mine in range(2):
            left = jnp.concatenate(
                [
                    panel(recv_ab, p, left_chunk, 0) if mine else panel(recv_a, p, left_chunk)
                    for p in range(half)
                ],
                axis=1,
            )
            product = contract_first(left, right)
            base = (near if mine else 1 - near) * half
            for q in range(half):
                at = q * lanes
                for p in range(half):
                    piece = product[at : at + width, p * lanes : (p + 1) * lanes]
                    for k in range(1, own):
                        low = at + k * width
                        piece = jnp.where(
                            group == k,
                            product[low : low + width, p * lanes : (p + 1) * lanes],
                            piece,
                        )
                    send_own[p, (base + q) * CHUNKS + left_chunk, chunk] = piece.astype(BF16)

    for chunk in range(CHUNKS):
        wait_ab(recv_sem, chunk)
        if chunk < CHUNKS - 1:
            for other in range(chunk + 1):
                pieces(chunk, other)
                if other < chunk:
                    pieces(other, chunk)
    last = CHUNKS - 1
    for chunk in range(last):
        pieces(last, chunk)
    for other in range(CHUNKS):
        pieces(other, last)
    start_own()

    wait_own(recv_sem)
    for chunk in range(CHUNKS):
        final = back(1, chunk, recv_own[:, chunk].astype(F32))
        out_ref[:, chunk * width : (chunk + 1) * width, :] = (
            jnp.transpose(final).reshape(tile_rows, width, channels).astype(BF16)
        )
    for chunk in range(CHUNKS):
        wait_sum(send_sem, chunk)
        wait_ab(send_sem, chunk)
    wait_own(send_sem)
    wait_k(send_sem)


def fused(row_count, col_count, *args):
    tile_rows, tile_cols, channels = args[0].shape
    devices = row_count * col_count
    hidden = args[-1].shape[1]
    half = col_count // 2
    owners = row_count * half
    width = tile_cols // CHUNKS
    lanes = hidden // owners * width
    pairs = tile_rows * width
    vmem = pl.BlockSpec(memory_space=pltpu.VMEM)
    return pl.pallas_call(
        functools.partial(fused_kernel, row_count, col_count),
        out_shape=jax.ShapeDtypeStruct(args[0].shape, BF16),
        in_specs=[pl.BlockSpec(memory_space=pl.ANY)] * len(args),
        out_specs=vmem,
        scratch_shapes=[pltpu.VMEM(arg.shape, arg.dtype) for arg in args]
        + [
            pltpu.SemaphoreType.DMA((len(args),)),
            pltpu.VMEM((CHUNKS, channels, pairs), F32),
            pltpu.VMEM((2, tile_rows * owners, lanes), F32),
            pltpu.VMEM((CHUNKS, channels, pairs), F32),
            pltpu.VMEM(args[4].shape[:0:-1], BF16),
            pltpu.VMEM(args[8].shape[:1] + args[8].shape[:0:-1], BF16),
            pltpu.VMEM((2, channels, lanes), F32),
            pltpu.VMEM((2, channels, lanes), F32),
            pltpu.VMEM((2, owners, lanes), F32),
            pltpu.VMEM((2, owners, lanes), F32),
            pltpu.VMEM((owners, CHUNKS, 2, tile_rows, lanes), BF16),
            pltpu.VMEM((owners, CHUNKS, 2, tile_rows, lanes), BF16),
            pltpu.VMEM((CHUNKS, owners, 2, tile_rows, lanes), BF16),
            pltpu.VMEM((CHUNKS, owners, tile_rows, lanes), BF16),
            pltpu.VMEM((CHUNKS, owners, 2, tile_rows, lanes), BF16),
            pltpu.VMEM((CHUNKS, col_count, row_count, tile_rows, lanes), BF16),
            pltpu.VMEM((CHUNKS, devices, tile_rows, lanes), BF16),
            pltpu.VMEM((half, row_count, CHUNKS, tile_rows, lanes), BF16),
            pltpu.VMEM((owners, CHUNKS, tile_rows, lanes), BF16),
            pltpu.SemaphoreType.DMA((5 * CHUNKS,)),
            pltpu.SemaphoreType.DMA((5 * CHUNKS,)),
        ],
        compiler_params=pltpu.CompilerParams(
            collective_id=0, has_side_effects=True, vmem_limit_bytes=16 << 20
        ),
    )(*[pltpu.with_memory_space_constraint(arg, pltpu.HBM) for arg in args])


def solution(mesh):
    row_count, col_count = mesh.shape["row"], mesh.shape["col"]
    devices = row_count * col_count

    def step(*args):
        tile_rows, tile_cols, channels = args[0].shape
        hidden = args[-1].shape[1]
        owners = devices // 2
        own = hidden // owners
        width = tile_cols // CHUNKS
        fits = (
            hidden % devices == 0
            and col_count % 2 == 0
            and tile_cols % CHUNKS == 0
            and own * width == 128
            and tile_rows == width
            and tile_rows % 16 == 0
            and tile_rows % own == 0
            and own & (own - 1) == 0
            and row_count & (row_count - 1) == 0
            and col_count & (col_count - 1) == 0
            and row_count * tile_rows == col_count * tile_cols
        )
        return fused(row_count, col_count, *args) if fits else on_device(*args)

    return jax.shard_map(
        step,
        mesh=mesh,
        in_specs=(P("row", "col", None), P("row", "col"), P(), P(), P(), P(), P(), P(), P()),
        out_specs=P("row", "col", None),
        check_vma=False,
    )
```

```python
import functools

import jax
import jax.numpy as jnp
from jax import lax
from jax.experimental import pallas as pl
from jax.experimental.pallas import tpu as pltpu
from jax.sharding import PartitionSpec as P

epsilon = 1e-05


def normalize(values, weight_scale, weight_shift, reduce_axis):
    average = jnp.mean(values, axis=reduce_axis, keepdims=True)
    centred = values - average
    spread = jnp.mean(centred * centred, axis=reduce_axis, keepdims=True)
    return centred * lax.rsqrt(spread + epsilon) * weight_scale + weight_shift


def contract(left_panel, right_panel, layer_index):
    if layer_index == 0:
        product = jnp.einsum(
            "cik,cjk->cij", left_panel, right_panel, preferred_element_type=jnp.float32
        )
    else:
        product = jnp.einsum(
            "cki,ckj->cij", left_panel, right_panel, preferred_element_type=jnp.float32
        )
    return product.astype(jnp.bfloat16)


def gated_panel(pair_ln, weights, first, hidden, mask_float):
    projected = jnp.einsum(
        "ijd,de->eij",
        pair_ln,
        weights[:, first : first + 2 * hidden],
        preferred_element_type=jnp.float32,
    )
    return (jax.nn.sigmoid(projected[:hidden]) * projected[hidden:] * mask_float).astype(
        jnp.bfloat16
    )


def on_device(
    pair_state,
    pair_mask,
    input_gain,
    input_bias,
    proj_weights,
    gate_weights,
    output_gain,
    output_bias,
    output_weights,
):
    tile_rows, tile_cols, channels = pair_state.shape
    hidden = output_weights.shape[1]
    row_count = lax.axis_size("row")
    col_count = lax.axis_size("col")
    per_device = hidden // (row_count * col_count)
    current = pair_state.astype(jnp.float32)
    mask_float = pair_mask.astype(jnp.float32)[None]
    for layer_index in range(2):
        pair_ln = normalize(current, input_gain[layer_index], input_bias[layer_index], -1).astype(
            jnp.bfloat16
        )
        left_panel = gated_panel(pair_ln, proj_weights[layer_index], 0, hidden, mask_float)
        right_panel = gated_panel(
            pair_ln, proj_weights[layer_index], 2 * hidden, hidden, mask_float
        )
        gate_value = jax.nn.sigmoid(
            jnp.einsum(
                "ijd,de->ije",
                pair_ln,
                gate_weights[layer_index],
                preferred_element_type=jnp.float32,
            )
        )
        scale_out = output_gain[layer_index]
        shift_out = output_bias[layer_index]
        weight_out = output_weights[layer_index]
        left_recv, right_recv = (
            lax.all_to_all(left_panel, ("row", "col"), split_axis=0, concat_axis=1, tiled=True),
            lax.all_to_all(right_panel, ("row", "col"), split_axis=0, concat_axis=1, tiled=True),
        )
        left_chan = (
            left_recv.reshape(per_device, row_count, col_count, tile_rows, tile_cols)
            .transpose(0, 1, 3, 2, 4)
            .reshape(per_device, row_count * tile_rows, col_count * tile_cols)
        )
        right_chan = (
            right_recv.reshape(per_device, row_count, col_count, tile_rows, tile_cols)
            .transpose(0, 1, 3, 2, 4)
            .reshape(per_device, row_count * tile_rows, col_count * tile_cols)
        )
        product = contract(left_chan, right_chan, layer_index)
        arranged = (
            product.reshape(per_device, row_count, tile_rows, col_count, tile_cols)
            .transpose(0, 1, 3, 2, 4)
            .reshape(per_device, row_count * col_count * tile_rows, tile_cols)
        )
        returned = lax.all_to_all(arranged, ("row", "col"), split_axis=1, concat_axis=0, tiled=True)
        normed = normalize(
            returned.astype(jnp.float32), scale_out[:, None, None], shift_out[:, None, None], 0
        ).astype(jnp.bfloat16)
        update = jnp.einsum("cij,cd->ijd", normed, weight_out, preferred_element_type=jnp.float32)
        current = current + gate_value * update
    return current.astype(jnp.bfloat16)


MESH = pl.DeviceIdType.MESH
F32 = jnp.float32
BF16 = jnp.bfloat16
CHUNKS = 2


def sigmoid(values):
    return 0.5 * jnp.tanh(0.5 * values) + 0.5


def lane_groups(shape, width):
    return lax.broadcasted_iota(jnp.int32, shape, len(shape) - 1) // width


def swap_groups(blocks, width):
    count = len(blocks)
    lanes = count * width
    group = lane_groups(blocks[0].shape, width)
    held = [pltpu.roll(part, at * width, 1) if at else part for at, part in enumerate(blocks)]
    step = 1
    while step < count:
        high = (group // step) % 2 == 1
        held = [jnp.where(high, held[(at + step) % count], held[at]) for at in range(count)]
        step *= 2
    return [
        pltpu.roll(held[-at % count], lanes - at * width, 1) if at else held[0]
        for at in range(count)
    ]


def columns_of(row_vector, lanes):
    return jnp.transpose(jnp.broadcast_to(row_vector, (lanes, row_vector.shape[1])))


def contract_first(left, right):
    return lax.dot_general(left, right, (((0,), (0,)), ((), ())), preferred_element_type=F32)


def fused_kernel(row_count, col_count, *refs):
    operands, out_ref, held = refs[:9], refs[9], refs[10:19]
    load_sem = refs[19]
    loads = [
        pltpu.make_async_copy(source, target, load_sem.at[at])
        for at, (source, target) in enumerate(zip(operands, held))
    ]
    for at in (0, 4, 2, 3, 1, 5, 6, 7, 8):
        loads[at].start()
    fused_body(row_count, col_count, loads, *held, out_ref, *refs[20:])


def fused_body(
    row_count,
    col_count,
    loads,
    z_ref,
    mask_ref,
    in_gain,
    in_bias,
    proj_ref,
    gate_ref,
    out_gain,
    out_bias,
    outw_ref,
    out_ref,
    zt_ref,
    tmp_ref,
    gated_ref,
    projt_ref,
    outwt_ref,
    in_gain_ref,
    in_bias_ref,
    gain_ref,
    bias_ref,
    send_k,
    recv_k,
    send_ab,
    recv_a,
    recv_ab,
    send_sum,
    recv_sum,
    send_own,
    recv_own,
    send_sem,
    recv_sem,
):
    tile_rows, tile_cols, channels = z_ref.shape
    devices = row_count * col_count
    hidden = outw_ref.shape[1]
    half = col_count // 2
    width = tile_cols // CHUNKS
    pairs = tile_rows * width
    owners = row_count * half
    own = hidden // owners
    lanes = own * width
    blocks = pairs // lanes
    tokens = row_count * tile_rows
    row, col = lax.axis_index("row"), lax.axis_index("col")
    near, inner = col // half, lax.rem(col, half)
    me = row * half + inner

    def flips(index, count):
        bits = count.bit_length() - 1
        moves = [(1 << b) * (1 - 2 * lax.rem(index // (1 << b), 2)) for b in range(bits)]

        def flipped(pattern):
            total = index
            for b in range(bits):
                if pattern >> b & 1:
                    total = total + moves[b]
            return total

        return [flipped(pattern) for pattern in range(count)]

    rows, cols = flips(row, row_count), flips(col, col_count)
    row_order = sorted(range(row_count), key=lambda p: (-p.bit_count(), -p))
    across = list(range(half, col_count))
    within = list(range(half - 1, -1, -1))

    def each(action, turns):
        for turn in turns:
            for step in row_order:
                if turn or step:
                    action(rows[step], cols[turn])

    barrier = pltpu.get_barrier_semaphore()

    def greet(trow, tcol):
        pl.semaphore_signal(barrier, inc=1, device_id=(trow, tcol), device_id_type=MESH)

    greet(row, cols[half])
    each(greet, within)

    def send(source, target, at, trow, tcol):
        pltpu.make_async_remote_copy(
            src_ref=source,
            dst_ref=target,
            send_sem=send_sem.at[at],
            recv_sem=recv_sem.at[at],
            device_id=(trow, tcol),
            device_id_type=MESH,
        ).start()

    def owner(trow, tcol):
        return trow * half + lax.rem(tcol, half)

    slot = inner * row_count + row

    def start_k():
        each(
            lambda trow, tcol: send(send_k.at[owner(trow, tcol)], recv_k.at[slot], 0, trow, tcol),
            within,
        )
        recv_k[slot] = send_k[me]

    def wait_k(sem):
        slots = recv_k.at[pl.ds(0, owners - 1)]
        pltpu.make_async_copy(slots, slots, sem.at[0]).wait()

    def start_sum(chunk):
        each(
            lambda trow, tcol: send(
                send_sum.at[chunk, tcol, trow],
                recv_sum.at[chunk, near * owners + me],
                CHUNKS + chunk,
                trow,
                tcol,
            ),
            (within + across if chunk else across + within),
        )
        recv_sum[chunk, near * owners + me] = send_sum[chunk, col, row]

    def wait_sum(sem, chunk):
        slots = recv_sum.at[chunk, pl.ds(0, devices - 1)]
        pltpu.make_async_copy(slots, slots, sem.at[CHUNKS + chunk]).wait()

    def start_a(chunk):
        each(
            lambda trow, tcol: send(
                send_ab.at[chunk, owner(trow, tcol), 0],
                recv_a.at[chunk, slot],
                2 * CHUNKS + chunk,
                trow,
                tcol,
            ),
            across[::-1] if chunk else across,
        )

    def start_ab(chunk):
        each(
            lambda trow, tcol: send(
                send_ab.at[chunk, owner(trow, tcol)],
                recv_ab.at[chunk, slot],
                3 * CHUNKS + chunk,
                trow,
                tcol,
            ),
            within,
        )
        recv_ab[chunk, slot] = send_ab[chunk, me]

    def wait_ab(sem, chunk):
        slots = recv_a.at[chunk]
        pltpu.make_async_copy(slots, slots, sem.at[2 * CHUNKS + chunk]).wait()
        slots = recv_ab.at[chunk, pl.ds(0, owners - 1)]
        pltpu.make_async_copy(slots, slots, sem.at[3 * CHUNKS + chunk]).wait()

    def start_own():
        each(
            lambda trow, tcol: send(
                send_own.at[lax.rem(tcol, half), trow], recv_own.at[me], 4 * CHUNKS, trow, tcol
            ),
            within,
        )
        recv_own[me] = send_own[inner, row]

    def wait_own(sem):
        slots = recv_own.at[pl.ds(0, owners - 1)]
        pltpu.make_async_copy(slots, slots, sem.at[4 * CHUNKS]).wait()

    def spread_inputs(layer):
        in_gain_ref[layer] = columns_of(in_gain[layer : layer + 1, :], lanes)
        in_bias_ref[layer] = columns_of(in_bias[layer : layer + 1, :], lanes)

    def spread_outputs(layer):
        group = lane_groups((owners, lanes), width)
        for source, kept in ((out_gain, gain_ref), (out_bias, bias_ref)):
            wide = columns_of(source[layer : layer + 1, :], lanes)
            packed = wide[0:owners]
            for k in range(1, own):
                packed = jnp.where(group == k, wide[k * owners : (k + 1) * owners], packed)
            kept[layer] = packed

    def front(layer, current, mask_flat, target_at, sent=None):
        centred = current - jnp.mean(current, axis=0, keepdims=True)
        scale = lax.rsqrt(jnp.mean(centred * centred, axis=0, keepdims=True) + epsilon)
        gain = jnp.concatenate([in_gain_ref[layer]] * blocks, axis=1)
        bias = jnp.concatenate([in_bias_ref[layer]] * blocks, axis=1)
        normed = (centred * scale * gain + bias).astype(BF16)
        for side in range(2):
            first = 2 * side * hidden
            if layer == 0:
                weights = proj_ref[layer, :, first : first + 2 * hidden]
                projected = contract_first(weights, normed)
            else:
                weights = projt_ref[first : first + 2 * hidden]
                projected = jnp.dot(weights, normed, preferred_element_type=F32)
            panel = (sigmoid(projected[:hidden]) * projected[hidden:] * mask_flat).astype(BF16)
            for block in range(blocks):
                parts = [
                    panel[k * owners : (k + 1) * owners, block * lanes : (block + 1) * lanes]
                    for k in range(own)
                ]
                for q, part in enumerate(swap_groups(parts, width)):
                    line = block * own + q
                    tmp_ref[side, line * owners : (line + 1) * owners, :] = part.astype(F32)
            for target in range(owners):
                target_at(target)[side] = tmp_ref[
                    side, pl.ds(target, tile_rows, stride=owners), :
                ].astype(BF16)
            if sent is not None:
                sent[side]()
        return normed

    def gate(layer, chunk, normed):
        gated_ref[chunk] = sigmoid(contract_first(gate_ref[layer], normed))

    def over_channels(values):
        total = jnp.sum(values, axis=0)
        shift = lanes // 2
        while shift >= width:
            total = total + pltpu.roll(total, shift, 1)
            shift //= 2
        return total * (1.0 / hidden)

    def back(layer, chunk, returned):
        centred = returned - over_channels(returned)[None]
        scale = lax.rsqrt(over_channels(centred * centred) + epsilon)
        for d in range(owners):
            tmp_ref[chunk, d * tile_rows : (d + 1) * tile_rows, :] = (
                centred[d] * scale * gain_ref[layer, d : d + 1, :] + bias_ref[layer, d : d + 1, :]
            )
        wide_blocks = []
        for block in range(blocks):
            parts = [
                tmp_ref[chunk, pl.ds(block * own + q, owners, stride=tile_rows), :] for q in range(own)
            ]
            wide_blocks.append(jnp.concatenate(swap_groups(parts, width), axis=0).astype(BF16))
        update = jnp.dot(
            outwt_ref[layer], jnp.concatenate(wide_blocks, axis=1), preferred_element_type=F32
        )
        return zt_ref[chunk] + gated_ref[chunk] * update

    for at in (2, 3):
        loads[at].wait()
    spread_inputs(0)
    loads[1].wait()
    mask_float = mask_ref[...].astype(F32)
    column = lax.broadcasted_iota(jnp.int32, (tile_cols, pairs), 1) % width
    mine = (
        lax.broadcasted_iota(jnp.int32, (tile_rows, pairs), 1) // width
        == lax.broadcasted_iota(jnp.int32, (tile_rows, pairs), 0)
    ).astype(F32)
    mask_flat = []
    for chunk in range(CHUNKS):
        spread = (
            column + chunk * width == lax.broadcasted_iota(jnp.int32, (tile_cols, pairs), 0)
        ).astype(F32)
        mask_flat.append(
            jnp.sum(
                jnp.dot(mask_float, spread, preferred_element_type=F32) * mine,
                axis=0,
                keepdims=True,
            )
        )
    loads[0].wait()
    loads[4].wait()
    normed = [None] * CHUNKS
    for chunk in range(CHUNKS):
        zt_ref[chunk] = jnp.transpose(
            z_ref[:, chunk * width : (chunk + 1) * width, :].astype(F32).reshape(pairs, channels)
        )
        normed[chunk] = front(
            0,
            zt_ref[chunk],
            mask_flat[chunk],
            lambda target, chunk=chunk: send_k.at[target, chunk],
        )
    pl.semaphore_wait(barrier, owners)
    start_k()
    for at in (5, 6, 7, 8):
        loads[at].wait()
    for layer in range(1, 2):
        projt_ref[...] = jnp.transpose(proj_ref[layer])
    for layer in range(2):
        outwt_ref[layer] = jnp.transpose(outw_ref[layer])
    for chunk in range(CHUNKS):
        gate(0, chunk, normed[chunk])
    spread_inputs(1)
    for layer in range(2):
        spread_outputs(layer)
    wait_k(recv_sem)

    def panel(ref, plane, *at):
        span = (slice(plane * row_count, (plane + 1) * row_count),)
        return ref[at[:1] + span + at[1:] if ref is not recv_k else span + at].reshape(tokens, lanes)

    spans = [(chunk, plane) for chunk in range(CHUNKS) for plane in range(half)]
    left = jnp.concatenate([panel(recv_k, p, c, 0) for c, p in spans], axis=1)
    right = jnp.concatenate([panel(recv_k, p, c, 1) for c, p in spans], axis=1)
    lane_group = lane_groups((1, len(spans) * lanes), width) % own
    masks = [(lane_group == k).astype(F32).astype(BF16) for k in range(own)]
    for chunk in range(CHUNKS):
        for c in range(col_count):
            at = (c * CHUNKS + chunk) * width
            lines = right[at : at + width]
            stacked = jnp.concatenate([lines * masks[k] for k in range(own)], axis=0)
            product = lax.dot_general(
                left, stacked, (((1,), (1,)), ((), ())), preferred_element_type=F32
            )
            send_sum[chunk, c] = product.astype(BF16).reshape(row_count, tile_rows, lanes)
        start_sum(chunk)

    for chunk in range(CHUNKS):
        wait_sum(recv_sem, chunk)
        returned = recv_sum[chunk, 0:owners].astype(F32) + recv_sum[
            chunk, owners : 2 * owners
        ].astype(F32)
        zt_ref[chunk] = back(0, chunk, returned)
        normed[chunk] = front(
            1,
            zt_ref[chunk],
            mask_flat[chunk],
            lambda target, chunk=chunk: send_ab.at[chunk, target],
            (lambda chunk=chunk: start_a(chunk), lambda chunk=chunk: start_ab(chunk)),
        )
    for chunk in range(CHUNKS):
        gate(1, chunk, normed[chunk])
    group = lane_groups((width, lanes), width)

    def pieces(left_chunk, chunk):
        right = jnp.concatenate([panel(recv_ab, p, chunk, 1) for p in range(half)], axis=1)
        for mine in range(2):
            left = jnp.concatenate(
                [
                    panel(recv_ab, p, left_chunk, 0) if mine else panel(recv_a, p, left_chunk)
                    for p in range(half)
                ],
                axis=1,
            )
            product = contract_first(left, right)
            base = (near if mine else 1 - near) * half
            for q in range(half):
                at = q * lanes
                for p in range(half):
                    piece = product[at : at + width, p * lanes : (p + 1) * lanes]
                    for k in range(1, own):
                        low = at + k * width
                        piece = jnp.where(
                            group == k,
                            product[low : low + width, p * lanes : (p + 1) * lanes],
                            piece,
                        )
                    send_own[p, (base + q) * CHUNKS + left_chunk, chunk] = piece.astype(BF16)

    for chunk in range(CHUNKS):
        wait_ab(recv_sem, chunk)
        if chunk < CHUNKS - 1:
            for other in range(chunk + 1):
                pieces(chunk, other)
                if other < chunk:
                    pieces(other, chunk)
    last = CHUNKS - 1
    for chunk in range(last):
        pieces(last, chunk)
    for other in range(CHUNKS):
        pieces(other, last)
    start_own()

    wait_own(recv_sem)
    for chunk in range(CHUNKS):
        final = back(1, chunk, recv_own[:, chunk].astype(F32))
        out_ref[:, chunk * width : (chunk + 1) * width, :] = (
            jnp.transpose(final).reshape(tile_rows, width, channels).astype(BF16)
        )
    for chunk in range(CHUNKS):
        wait_sum(send_sem, chunk)
        wait_ab(send_sem, chunk)
    wait_own(send_sem)
    wait_k(send_sem)


def fused(row_count, col_count, *args):
    tile_rows, tile_cols, channels = args[0].shape
    devices = row_count * col_count
    hidden = args[-1].shape[1]
    half = col_count // 2
    owners = row_count * half
    width = tile_cols // CHUNKS
    lanes = hidden // owners * width
    pairs = tile_rows * width
    vmem = pl.BlockSpec(memory_space=pltpu.VMEM)
    return pl.pallas_call(
        functools.partial(fused_kernel, row_count, col_count),
        out_shape=jax.ShapeDtypeStruct(args[0].shape, BF16),
        in_specs=[pl.BlockSpec(memory_space=pl.ANY)] * len(args),
        out_specs=vmem,
        scratch_shapes=[pltpu.VMEM(arg.shape, arg.dtype) for arg in args]
        + [
            pltpu.SemaphoreType.DMA((len(args),)),
            pltpu.VMEM((CHUNKS, channels, pairs), F32),
            pltpu.VMEM((2, tile_rows * owners, lanes), F32),
            pltpu.VMEM((CHUNKS, channels, pairs), F32),
            pltpu.VMEM(args[4].shape[:0:-1], BF16),
            pltpu.VMEM(args[8].shape[:1] + args[8].shape[:0:-1], BF16),
            pltpu.VMEM((2, channels, lanes), F32),
            pltpu.VMEM((2, channels, lanes), F32),
            pltpu.VMEM((2, owners, lanes), F32),
            pltpu.VMEM((2, owners, lanes), F32),
            pltpu.VMEM((owners, CHUNKS, 2, tile_rows, lanes), BF16),
            pltpu.VMEM((owners, CHUNKS, 2, tile_rows, lanes), BF16),
            pltpu.VMEM((CHUNKS, owners, 2, tile_rows, lanes), BF16),
            pltpu.VMEM((CHUNKS, owners, tile_rows, lanes), BF16),
            pltpu.VMEM((CHUNKS, owners, 2, tile_rows, lanes), BF16),
            pltpu.VMEM((CHUNKS, col_count, row_count, tile_rows, lanes), BF16),
            pltpu.VMEM((CHUNKS, devices, tile_rows, lanes), BF16),
            pltpu.VMEM((half, row_count, CHUNKS, tile_rows, lanes), BF16),
            pltpu.VMEM((owners, CHUNKS, tile_rows, lanes), BF16),
            pltpu.SemaphoreType.DMA((5 * CHUNKS,)),
            pltpu.SemaphoreType.DMA((5 * CHUNKS,)),
        ],
        compiler_params=pltpu.CompilerParams(
            collective_id=0, has_side_effects=True, vmem_limit_bytes=16 << 20
        ),
    )(*[pltpu.with_memory_space_constraint(arg, pltpu.HBM) for arg in args])


def solution(mesh):
    row_count, col_count = mesh.shape["row"], mesh.shape["col"]
    devices = row_count * col_count

    def step(*args):
        tile_rows, tile_cols, channels = args[0].shape
        hidden = args[-1].shape[1]
        owners = devices // 2
        own = hidden // owners
        width = tile_cols // CHUNKS
        fits = (
            hidden % devices == 0
            and col_count % 2 == 0
            and tile_cols % CHUNKS == 0
            and own * width == 128
            and tile_rows == width
            and tile_rows % 16 == 0
            and tile_rows % own == 0
            and own & (own - 1) == 0
            and row_count & (row_count - 1) == 0
            and col_count & (col_count - 1) == 0
            and row_count * tile_rows == col_count * tile_cols
        )
        return fused(row_count, col_count, *args) if fits else on_device(*args)

    return jax.shard_map(
        step,
        mesh=mesh,
        in_specs=(P("row", "col", None), P("row", "col"), P(), P(), P(), P(), P(), P(), P()),
        out_specs=P("row", "col", None),
        check_vma=False,
    )
```

```python
import functools

import jax
import jax.numpy as jnp
from jax import lax
from jax.experimental import pallas as pl
from jax.experimental.pallas import tpu as pltpu
from jax.sharding import PartitionSpec as P

epsilon = 1e-05


def normalize(values, weight_scale, weight_shift, reduce_axis):
    average = jnp.mean(values, axis=reduce_axis, keepdims=True)
    centred = values - average
    spread = jnp.mean(centred * centred, axis=reduce_axis, keepdims=True)
    return centred * lax.rsqrt(spread + epsilon) * weight_scale + weight_shift


def contract(left_panel, right_panel, layer_index):
    if layer_index == 0:
        product = jnp.einsum(
            "cik,cjk->cij", left_panel, right_panel, preferred_element_type=jnp.float32
        )
    else:
        product = jnp.einsum(
            "cki,ckj->cij", left_panel, right_panel, preferred_element_type=jnp.float32
        )
    return product.astype(jnp.bfloat16)


def gated_panel(pair_ln, weights, first, hidden, mask_float):
    projected = jnp.einsum(
        "ijd,de->eij",
        pair_ln,
        weights[:, first : first + 2 * hidden],
        preferred_element_type=jnp.float32,
    )
    return (jax.nn.sigmoid(projected[:hidden]) * projected[hidden:] * mask_float).astype(
        jnp.bfloat16
    )


def on_device(
    pair_state,
    pair_mask,
    input_gain,
    input_bias,
    proj_weights,
    gate_weights,
    output_gain,
    output_bias,
    output_weights,
):
    tile_rows, tile_cols, channels = pair_state.shape
    hidden = output_weights.shape[1]
    row_count = lax.axis_size("row")
    col_count = lax.axis_size("col")
    per_device = hidden // (row_count * col_count)
    current = pair_state.astype(jnp.float32)
    mask_float = pair_mask.astype(jnp.float32)[None]
    for layer_index in range(2):
        pair_ln = normalize(current, input_gain[layer_index], input_bias[layer_index], -1).astype(
            jnp.bfloat16
        )
        left_panel = gated_panel(pair_ln, proj_weights[layer_index], 0, hidden, mask_float)
        right_panel = gated_panel(
            pair_ln, proj_weights[layer_index], 2 * hidden, hidden, mask_float
        )
        gate_value = jax.nn.sigmoid(
            jnp.einsum(
                "ijd,de->ije",
                pair_ln,
                gate_weights[layer_index],
                preferred_element_type=jnp.float32,
            )
        )
        scale_out = output_gain[layer_index]
        shift_out = output_bias[layer_index]
        weight_out = output_weights[layer_index]
        left_recv, right_recv = (
            lax.all_to_all(left_panel, ("row", "col"), split_axis=0, concat_axis=1, tiled=True),
            lax.all_to_all(right_panel, ("row", "col"), split_axis=0, concat_axis=1, tiled=True),
        )
        left_chan = (
            left_recv.reshape(per_device, row_count, col_count, tile_rows, tile_cols)
            .transpose(0, 1, 3, 2, 4)
            .reshape(per_device, row_count * tile_rows, col_count * tile_cols)
        )
        right_chan = (
            right_recv.reshape(per_device, row_count, col_count, tile_rows, tile_cols)
            .transpose(0, 1, 3, 2, 4)
            .reshape(per_device, row_count * tile_rows, col_count * tile_cols)
        )
        product = contract(left_chan, right_chan, layer_index)
        arranged = (
            product.reshape(per_device, row_count, tile_rows, col_count, tile_cols)
            .transpose(0, 1, 3, 2, 4)
            .reshape(per_device, row_count * col_count * tile_rows, tile_cols)
        )
        returned = lax.all_to_all(arranged, ("row", "col"), split_axis=1, concat_axis=0, tiled=True)
        normed = normalize(
            returned.astype(jnp.float32), scale_out[:, None, None], shift_out[:, None, None], 0
        ).astype(jnp.bfloat16)
        update = jnp.einsum("cij,cd->ijd", normed, weight_out, preferred_element_type=jnp.float32)
        current = current + gate_value * update
    return current.astype(jnp.bfloat16)


MESH = pl.DeviceIdType.MESH
F32 = jnp.float32
BF16 = jnp.bfloat16
CHUNKS = 2


def sigmoid(values):
    return 0.5 * jnp.tanh(0.5 * values) + 0.5


def lane_groups(shape, width):
    return lax.broadcasted_iota(jnp.int32, shape, len(shape) - 1) // width


def swap_groups(blocks, width):
    count = len(blocks)
    lanes = count * width
    group = lane_groups(blocks[0].shape, width)
    held = [pltpu.roll(part, at * width, 1) if at else part for at, part in enumerate(blocks)]
    step = 1
    while step < count:
        high = (group // step) % 2 == 1
        held = [jnp.where(high, held[(at + step) % count], held[at]) for at in range(count)]
        step *= 2
    return [
        pltpu.roll(held[-at % count], lanes - at * width, 1) if at else held[0]
        for at in range(count)
    ]


def columns_of(row_vector, lanes):
    return jnp.transpose(jnp.broadcast_to(row_vector, (lanes, row_vector.shape[1])))


def contract_first(left, right):
    return lax.dot_general(left, right, (((0,), (0,)), ((), ())), preferred_element_type=F32)


def fused_kernel(row_count, col_count, *refs):
    operands, out_ref, held = refs[:9], refs[9], refs[10:19]
    load_sem = refs[19]
    loads = [
        pltpu.make_async_copy(source, target, load_sem.at[at])
        for at, (source, target) in enumerate(zip(operands, held))
    ]
    for at in (0, 4, 2, 3, 1, 5, 6, 7, 8):
        loads[at].start()
    fused_body(row_count, col_count, loads, *held, out_ref, *refs[20:])


def fused_body(
    row_count,
    col_count,
    loads,
    z_ref,
    mask_ref,
    in_gain,
    in_bias,
    proj_ref,
    gate_ref,
    out_gain,
    out_bias,
    outw_ref,
    out_ref,
    zt_ref,
    tmp_ref,
    gated_ref,
    flat_ref,
    gated_flat_ref,
    projt_ref,
    outwt_ref,
    in_gain_ref,
    in_bias_ref,
    gain_ref,
    bias_ref,
    send_k,
    recv_k,
    send_ab,
    recv_a,
    recv_ab,
    send_sum,
    recv_sum,
    send_own,
    recv_own,
    send_sem,
    recv_sem,
):
    tile_rows, tile_cols, channels = z_ref.shape
    devices = row_count * col_count
    hidden = outw_ref.shape[1]
    half = col_count // 2
    width = tile_cols // CHUNKS
    pairs = tile_rows * width
    owners = row_count * half
    own = hidden // owners
    lanes = own * width
    blocks = pairs // lanes
    tokens = row_count * tile_rows
    row, col = lax.axis_index("row"), lax.axis_index("col")
    near, inner = col // half, lax.rem(col, half)
    me = row * half + inner

    def flips(index, count):
        bits = count.bit_length() - 1
        moves = [(1 << b) * (1 - 2 * lax.rem(index // (1 << b), 2)) for b in range(bits)]

        def flipped(pattern):
            total = index
            for b in range(bits):
                if pattern >> b & 1:
                    total = total + moves[b]
            return total

        return [flipped(pattern) for pattern in range(count)]

    rows, cols = flips(row, row_count), flips(col, col_count)
    row_order = sorted(range(row_count), key=lambda p: (-p.bit_count(), -p))
    across = list(range(half, col_count))
    within = list(range(half - 1, -1, -1))

    def each(action, turns):
        for turn in turns:
            for step in row_order:
                if turn or step:
                    action(rows[step], cols[turn])

    barrier = pltpu.get_barrier_semaphore()

    def greet(trow, tcol):
        pl.semaphore_signal(barrier, inc=1, device_id=(trow, tcol), device_id_type=MESH)

    greet(row, cols[half])
    each(greet, within)

    def send(source, target, at, trow, tcol):
        pltpu.make_async_remote_copy(
            src_ref=source,
            dst_ref=target,
            send_sem=send_sem.at[at],
            recv_sem=recv_sem.at[at],
            device_id=(trow, tcol),
            device_id_type=MESH,
        ).start()

    def owner(trow, tcol):
        return trow * half + lax.rem(tcol, half)

    slot = inner * row_count + row

    def start_k():
        each(
            lambda trow, tcol: send(send_k.at[owner(trow, tcol)], recv_k.at[slot], 0, trow, tcol),
            within,
        )
        recv_k[slot] = send_k[me]

    def wait_k(sem):
        slots = recv_k.at[pl.ds(0, owners - 1)]
        pltpu.make_async_copy(slots, slots, sem.at[0]).wait()

    def start_sum(chunk):
        each(
            lambda trow, tcol: send(
                send_sum.at[chunk, tcol, trow],
                recv_sum.at[chunk, near * owners + me],
                CHUNKS + chunk,
                trow,
                tcol,
            ),
            (within + across if chunk else across + within),
        )
        recv_sum[chunk, near * owners + me] = send_sum[chunk, col, row]

    def wait_sum(sem, chunk):
        slots = recv_sum.at[chunk, pl.ds(0, devices - 1)]
        pltpu.make_async_copy(slots, slots, sem.at[CHUNKS + chunk]).wait()

    def start_a(chunk):
        each(
            lambda trow, tcol: send(
                send_ab.at[chunk, owner(trow, tcol), 0],
                recv_a.at[chunk, slot],
                2 * CHUNKS + chunk,
                trow,
                tcol,
            ),
            across[::-1] if chunk else across,
        )

    def start_ab(chunk):
        each(
            lambda trow, tcol: send(
                send_ab.at[chunk, owner(trow, tcol)],
                recv_ab.at[chunk, slot],
                3 * CHUNKS + chunk,
                trow,
                tcol,
            ),
            within,
        )
        recv_ab[chunk, slot] = send_ab[chunk, me]

    def wait_ab(sem, chunk):
        slots = recv_a.at[chunk]
        pltpu.make_async_copy(slots, slots, sem.at[2 * CHUNKS + chunk]).wait()
        slots = recv_ab.at[chunk, pl.ds(0, owners - 1)]
        pltpu.make_async_copy(slots, slots, sem.at[3 * CHUNKS + chunk]).wait()

    def start_own():
        each(
            lambda trow, tcol: send(
                send_own.at[lax.rem(tcol, half), trow], recv_own.at[me], 4 * CHUNKS, trow, tcol
            ),
            within,
        )
        recv_own[me] = send_own[inner, row]

    def wait_own(sem):
        slots = recv_own.at[pl.ds(0, owners - 1)]
        pltpu.make_async_copy(slots, slots, sem.at[4 * CHUNKS]).wait()

    def spread_inputs(layer):
        in_gain_ref[layer] = columns_of(in_gain[layer : layer + 1, :], lanes)
        in_bias_ref[layer] = columns_of(in_bias[layer : layer + 1, :], lanes)

    def spread_outputs(layer):
        group = lane_groups((owners, lanes), width)
        for source, kept in ((out_gain, gain_ref), (out_bias, bias_ref)):
            wide = columns_of(source[layer : layer + 1, :], lanes)
            packed = wide[0:owners]
            for k in range(1, own):
                packed = jnp.where(group == k, wide[k * owners : (k + 1) * owners], packed)
            kept[layer] = packed

    def front(layer, current, mask_flat, target_at, sent=None):
        centred = current - jnp.mean(current, axis=0, keepdims=True)
        scale = lax.rsqrt(jnp.mean(centred * centred, axis=0, keepdims=True) + epsilon)
        gain = jnp.concatenate([in_gain_ref[layer]] * blocks, axis=1)
        bias = jnp.concatenate([in_bias_ref[layer]] * blocks, axis=1)
        normed = (centred * scale * gain + bias).astype(BF16)
        for side in range(2):
            first = 2 * side * hidden
            if layer == 0:
                weights = proj_ref[layer, :, first : first + 2 * hidden]
                projected = contract_first(weights, normed)
            else:
                weights = projt_ref[first : first + 2 * hidden]
                projected = jnp.dot(weights, normed, preferred_element_type=F32)
            panel = (sigmoid(projected[:hidden]) * projected[hidden:] * mask_flat).astype(BF16)
            for block in range(blocks):
                parts = [
                    panel[k * owners : (k + 1) * owners, block * lanes : (block + 1) * lanes]
                    for k in range(own)
                ]
                for q, part in enumerate(swap_groups(parts, width)):
                    line = block * own + q
                    tmp_ref[side, line * owners : (line + 1) * owners, :] = part.astype(F32)
            for target in range(owners):
                target_at(target)[side] = tmp_ref[
                    side, pl.ds(target, tile_rows, stride=owners), :
                ].astype(BF16)
            if sent is not None:
                sent[side]()
        return normed

    def gate(layer, chunk, normed):
        gated_ref[chunk] = sigmoid(contract_first(gate_ref[layer], normed))

    def over_channels(values):
        total = jnp.sum(values, axis=0)
        shift = lanes // 2
        while shift >= width:
            total = total + pltpu.roll(total, shift, 1)
            shift //= 2
        return total * (1.0 / hidden)

    def back(layer, chunk, returned):
        centred = returned - over_channels(returned)[None]
        scale = lax.rsqrt(over_channels(centred * centred) + epsilon)
        for d in range(owners):
            tmp_ref[chunk, d * tile_rows : (d + 1) * tile_rows, :] = (
                centred[d] * scale * gain_ref[layer, d : d + 1, :] + bias_ref[layer, d : d + 1, :]
            )
        wide_blocks = []
        for block in range(blocks):
            parts = [
                tmp_ref[chunk, pl.ds(block * own + q, owners, stride=tile_rows), :] for q in range(own)
            ]
            wide_blocks.append(jnp.concatenate(swap_groups(parts, width), axis=0).astype(BF16))
        wide = jnp.concatenate(wide_blocks, axis=1)
        if layer == 1:
            return flat_ref[chunk] + gated_flat_ref[chunk] * contract_first(wide, outw_ref[layer])
        update = jnp.dot(outwt_ref[layer], wide, preferred_element_type=F32)
        return zt_ref[chunk] + gated_ref[chunk] * update

    for at in (2, 3):
        loads[at].wait()
    spread_inputs(0)
    loads[1].wait()
    mask_float = mask_ref[...].astype(F32)
    column = lax.broadcasted_iota(jnp.int32, (tile_cols, pairs), 1) % width
    mine = (
        lax.broadcasted_iota(jnp.int32, (tile_rows, pairs), 1) // width
        == lax.broadcasted_iota(jnp.int32, (tile_rows, pairs), 0)
    ).astype(F32)
    mask_flat = []
    for chunk in range(CHUNKS):
        spread = (
            column + chunk * width == lax.broadcasted_iota(jnp.int32, (tile_cols, pairs), 0)
        ).astype(F32)
        mask_flat.append(
            jnp.sum(
                jnp.dot(mask_float, spread, preferred_element_type=F32) * mine,
                axis=0,
                keepdims=True,
            )
        )
    loads[0].wait()
    loads[4].wait()
    normed = [None] * CHUNKS
    for chunk in range(CHUNKS):
        zt_ref[chunk] = jnp.transpose(
            z_ref[:, chunk * width : (chunk + 1) * width, :].astype(F32).reshape(pairs, channels)
        )
        normed[chunk] = front(
            0,
            zt_ref[chunk],
            mask_flat[chunk],
            lambda target, chunk=chunk: send_k.at[target, chunk],
        )
    pl.semaphore_wait(barrier, owners)
    start_k()
    for at in (5, 6, 7, 8):
        loads[at].wait()
    for layer in range(1, 2):
        projt_ref[...] = jnp.transpose(proj_ref[layer])
    for layer in range(2):
        outwt_ref[layer] = jnp.transpose(outw_ref[layer])
    for chunk in range(CHUNKS):
        gate(0, chunk, normed[chunk])
    spread_inputs(1)
    for layer in range(2):
        spread_outputs(layer)
    wait_k(recv_sem)

    def panel(ref, plane, *at):
        span = (slice(plane * row_count, (plane + 1) * row_count),)
        return ref[at[:1] + span + at[1:] if ref is not recv_k else span + at].reshape(tokens, lanes)

    spans = [(chunk, plane) for chunk in range(CHUNKS) for plane in range(half)]
    lane_group = lane_groups((1, len(spans) * lanes), width) % own

    def sums(chunk):
        left = jnp.concatenate([panel(recv_k, p, c, 0) for c, p in spans], axis=1)
        right = jnp.concatenate([panel(recv_k, p, c, 1) for c, p in spans], axis=1)
        masks = [(lane_group == k).astype(F32).astype(BF16) for k in range(own)]
        for c in range(col_count):
            at = (c * CHUNKS + chunk) * width
            lines = right[at : at + width]
            stacked = jnp.concatenate([lines * masks[k] for k in range(own)], axis=0)
            product = lax.dot_general(
                left, stacked, (((1,), (1,)), ((), ())), preferred_element_type=F32
            )
            send_sum[chunk, c] = product.astype(BF16).reshape(row_count, tile_rows, lanes)
        start_sum(chunk)

    sums(0)
    for chunk in range(1, CHUNKS):
        pl.when(row >= 0)(lambda chunk=chunk: sums(chunk))

    for chunk in range(CHUNKS):
        wait_sum(recv_sem, chunk)
        returned = recv_sum[chunk, 0:owners].astype(F32) + recv_sum[
            chunk, owners : 2 * owners
        ].astype(F32)
        zt_ref[chunk] = back(0, chunk, returned)
        normed[chunk] = front(
            1,
            zt_ref[chunk],
            mask_flat[chunk],
            lambda target, chunk=chunk: send_ab.at[chunk, target],
            (
                (lambda chunk=chunk: start_a(chunk), lambda chunk=chunk: start_ab(chunk))
                if chunk < CHUNKS - 1
                else (lambda: None, lambda chunk=chunk: (start_a(chunk), start_ab(chunk)))
            ),
        )
    for chunk in range(CHUNKS):
        gated_flat_ref[chunk] = sigmoid(contract_first(normed[chunk], gate_ref[1]))
        flat_ref[chunk] = jnp.transpose(zt_ref[chunk])
    group = lane_groups((width, lanes), width)

    def pieces(left_chunk, chunk):
        right = jnp.concatenate([panel(recv_ab, p, chunk, 1) for p in range(half)], axis=1)
        for mine in range(2):
            left = jnp.concatenate(
                [
                    panel(recv_ab, p, left_chunk, 0) if mine else panel(recv_a, p, left_chunk)
                    for p in range(half)
                ],
                axis=1,
            )
            product = contract_first(left, right)
            base = (near if mine else 1 - near) * half
            for q in range(half):
                at = q * lanes
                for p in range(half):
                    piece = product[at : at + width, p * lanes : (p + 1) * lanes]
                    for k in range(1, own):
                        low = at + k * width
                        piece = jnp.where(
                            group == k,
                            product[low : low + width, p * lanes : (p + 1) * lanes],
                            piece,
                        )
                    send_own[p, (base + q) * CHUNKS + left_chunk, chunk] = piece.astype(BF16)

    for chunk in range(CHUNKS):
        wait_ab(recv_sem, chunk)
        if chunk < CHUNKS - 1:
            for other in range(chunk + 1):
                pieces(chunk, other)
                if other < chunk:
                    pieces(other, chunk)
    last = CHUNKS - 1
    for chunk in range(last):
        pieces(last, chunk)
    for other in range(CHUNKS):
        pieces(other, last)
    start_own()

    wait_own(recv_sem)
    for chunk in range(CHUNKS):
        final = back(1, chunk, recv_own[:, chunk].astype(F32))
        out_ref[:, chunk * width : (chunk + 1) * width, :] = (
            final.reshape(tile_rows, width, channels).astype(BF16)
        )
    for chunk in range(CHUNKS):
        wait_sum(send_sem, chunk)
        wait_ab(send_sem, chunk)
    wait_own(send_sem)
    wait_k(send_sem)


def fused(row_count, col_count, *args):
    tile_rows, tile_cols, channels = args[0].shape
    devices = row_count * col_count
    hidden = args[-1].shape[1]
    half = col_count // 2
    owners = row_count * half
    width = tile_cols // CHUNKS
    lanes = hidden // owners * width
    pairs = tile_rows * width
    vmem = pl.BlockSpec(memory_space=pltpu.VMEM)
    return pl.pallas_call(
        functools.partial(fused_kernel, row_count, col_count),
        out_shape=jax.ShapeDtypeStruct(args[0].shape, BF16),
        in_specs=[pl.BlockSpec(memory_space=pl.ANY)] * len(args),
        out_specs=vmem,
        scratch_shapes=[pltpu.VMEM(arg.shape, arg.dtype) for arg in args]
        + [
            pltpu.SemaphoreType.DMA((len(args),)),
            pltpu.VMEM((CHUNKS, channels, pairs), F32),
            pltpu.VMEM((2, tile_rows * owners, lanes), F32),
            pltpu.VMEM((CHUNKS, channels, pairs), F32),
            pltpu.VMEM((CHUNKS, pairs, channels), F32),
            pltpu.VMEM((CHUNKS, pairs, channels), F32),
            pltpu.VMEM(args[4].shape[:0:-1], BF16),
            pltpu.VMEM(args[8].shape[:1] + args[8].shape[:0:-1], BF16),
            pltpu.VMEM((2, channels, lanes), F32),
            pltpu.VMEM((2, channels, lanes), F32),
            pltpu.VMEM((2, owners, lanes), F32),
            pltpu.VMEM((2, owners, lanes), F32),
            pltpu.VMEM((owners, CHUNKS, 2, tile_rows, lanes), BF16),
            pltpu.VMEM((owners, CHUNKS, 2, tile_rows, lanes), BF16),
            pltpu.VMEM((CHUNKS, owners, 2, tile_rows, lanes), BF16),
            pltpu.VMEM((CHUNKS, owners, tile_rows, lanes), BF16),
            pltpu.VMEM((CHUNKS, owners, 2, tile_rows, lanes), BF16),
            pltpu.VMEM((CHUNKS, col_count, row_count, tile_rows, lanes), BF16),
            pltpu.VMEM((CHUNKS, devices, tile_rows, lanes), BF16),
            pltpu.VMEM((half, row_count, CHUNKS, tile_rows, lanes), BF16),
            pltpu.VMEM((owners, CHUNKS, tile_rows, lanes), BF16),
            pltpu.SemaphoreType.DMA((5 * CHUNKS,)),
            pltpu.SemaphoreType.DMA((5 * CHUNKS,)),
        ],
        compiler_params=pltpu.CompilerParams(
            collective_id=0, has_side_effects=True, vmem_limit_bytes=16 << 20
        ),
    )(*[pltpu.with_memory_space_constraint(arg, pltpu.HBM) for arg in args])


def solution(mesh):
    row_count, col_count = mesh.shape["row"], mesh.shape["col"]
    devices = row_count * col_count

    def step(*args):
        tile_rows, tile_cols, channels = args[0].shape
        hidden = args[-1].shape[1]
        owners = devices // 2
        own = hidden // owners
        width = tile_cols // CHUNKS
        fits = (
            hidden % devices == 0
            and col_count % 2 == 0
            and tile_cols % CHUNKS == 0
            and own * width == 128
            and tile_rows == width
            and tile_rows % 16 == 0
            and tile_rows % own == 0
            and own & (own - 1) == 0
            and row_count & (row_count - 1) == 0
            and col_count & (col_count - 1) == 0
            and row_count * tile_rows == col_count * tile_cols
        )
        return fused(row_count, col_count, *args) if fits else on_device(*args)

    return jax.shard_map(
        step,
        mesh=mesh,
        in_specs=(P("row", "col", None), P("row", "col"), P(), P(), P(), P(), P(), P(), P()),
        out_specs=P("row", "col", None),
        check_vma=False,
    )
```

```python
import functools

import jax
import jax.numpy as jnp
from jax import lax
from jax.experimental import pallas as pl
from jax.experimental.pallas import tpu as pltpu
from jax.sharding import PartitionSpec as P

epsilon = 1e-05


def normalize(values, weight_scale, weight_shift, reduce_axis):
    average = jnp.mean(values, axis=reduce_axis, keepdims=True)
    centred = values - average
    spread = jnp.mean(centred * centred, axis=reduce_axis, keepdims=True)
    return centred * lax.rsqrt(spread + epsilon) * weight_scale + weight_shift


def contract(left_panel, right_panel, layer_index):
    if layer_index == 0:
        product = jnp.einsum(
            "cik,cjk->cij", left_panel, right_panel, preferred_element_type=jnp.float32
        )
    else:
        product = jnp.einsum(
            "cki,ckj->cij", left_panel, right_panel, preferred_element_type=jnp.float32
        )
    return product.astype(jnp.bfloat16)


def gated_panel(pair_ln, weights, first, hidden, mask_float):
    projected = jnp.einsum(
        "ijd,de->eij",
        pair_ln,
        weights[:, first : first + 2 * hidden],
        preferred_element_type=jnp.float32,
    )
    return (jax.nn.sigmoid(projected[:hidden]) * projected[hidden:] * mask_float).astype(
        jnp.bfloat16
    )


def on_device(
    pair_state,
    pair_mask,
    input_gain,
    input_bias,
    proj_weights,
    gate_weights,
    output_gain,
    output_bias,
    output_weights,
):
    tile_rows, tile_cols, channels = pair_state.shape
    hidden = output_weights.shape[1]
    row_count = lax.axis_size("row")
    col_count = lax.axis_size("col")
    per_device = hidden // (row_count * col_count)
    current = pair_state.astype(jnp.float32)
    mask_float = pair_mask.astype(jnp.float32)[None]
    for layer_index in range(2):
        pair_ln = normalize(current, input_gain[layer_index], input_bias[layer_index], -1).astype(
            jnp.bfloat16
        )
        left_panel = gated_panel(pair_ln, proj_weights[layer_index], 0, hidden, mask_float)
        right_panel = gated_panel(
            pair_ln, proj_weights[layer_index], 2 * hidden, hidden, mask_float
        )
        gate_value = jax.nn.sigmoid(
            jnp.einsum(
                "ijd,de->ije",
                pair_ln,
                gate_weights[layer_index],
                preferred_element_type=jnp.float32,
            )
        )
        scale_out = output_gain[layer_index]
        shift_out = output_bias[layer_index]
        weight_out = output_weights[layer_index]
        left_recv, right_recv = (
            lax.all_to_all(left_panel, ("row", "col"), split_axis=0, concat_axis=1, tiled=True),
            lax.all_to_all(right_panel, ("row", "col"), split_axis=0, concat_axis=1, tiled=True),
        )
        left_chan = (
            left_recv.reshape(per_device, row_count, col_count, tile_rows, tile_cols)
            .transpose(0, 1, 3, 2, 4)
            .reshape(per_device, row_count * tile_rows, col_count * tile_cols)
        )
        right_chan = (
            right_recv.reshape(per_device, row_count, col_count, tile_rows, tile_cols)
            .transpose(0, 1, 3, 2, 4)
            .reshape(per_device, row_count * tile_rows, col_count * tile_cols)
        )
        product = contract(left_chan, right_chan, layer_index)
        arranged = (
            product.reshape(per_device, row_count, tile_rows, col_count, tile_cols)
            .transpose(0, 1, 3, 2, 4)
            .reshape(per_device, row_count * col_count * tile_rows, tile_cols)
        )
        returned = lax.all_to_all(arranged, ("row", "col"), split_axis=1, concat_axis=0, tiled=True)
        normed = normalize(
            returned.astype(jnp.float32), scale_out[:, None, None], shift_out[:, None, None], 0
        ).astype(jnp.bfloat16)
        update = jnp.einsum("cij,cd->ijd", normed, weight_out, preferred_element_type=jnp.float32)
        current = current + gate_value * update
    return current.astype(jnp.bfloat16)


MESH = pl.DeviceIdType.MESH
F32 = jnp.float32
BF16 = jnp.bfloat16
CHUNKS = 2


def sigmoid(values):
    return 0.5 * jnp.tanh(0.5 * values) + 0.5


def lane_groups(shape, width):
    return lax.broadcasted_iota(jnp.int32, shape, len(shape) - 1) // width


def swap_groups(blocks, width):
    count = len(blocks)
    lanes = count * width
    group = lane_groups(blocks[0].shape, width)
    held = [pltpu.roll(part, at * width, 1) if at else part for at, part in enumerate(blocks)]
    step = 1
    while step < count:
        high = (group // step) % 2 == 1
        held = [jnp.where(high, held[(at + step) % count], held[at]) for at in range(count)]
        step *= 2
    return [
        pltpu.roll(held[-at % count], lanes - at * width, 1) if at else held[0]
        for at in range(count)
    ]


def columns_of(row_vector, lanes):
    return jnp.transpose(jnp.broadcast_to(row_vector, (lanes, row_vector.shape[1])))


def contract_first(left, right):
    return lax.dot_general(left, right, (((0,), (0,)), ((), ())), preferred_element_type=F32)


def fused_kernel(row_count, col_count, *refs):
    operands, out_ref, held = refs[:9], refs[9], refs[10:19]
    load_sem = refs[19]
    loads = [
        pltpu.make_async_copy(source, target, load_sem.at[at])
        for at, (source, target) in enumerate(zip(operands, held))
    ]
    for at in (0, 4, 2, 3, 1, 5, 6, 7, 8):
        loads[at].start()
    fused_body(row_count, col_count, loads, *held, out_ref, *refs[20:])


def fused_body(
    row_count,
    col_count,
    loads,
    z_ref,
    mask_ref,
    in_gain,
    in_bias,
    proj_ref,
    gate_ref,
    out_gain,
    out_bias,
    outw_ref,
    out_ref,
    zt_ref,
    tmp_ref,
    gated_ref,
    flat_ref,
    gated_flat_ref,
    projt_ref,
    outwt_ref,
    in_gain_ref,
    in_bias_ref,
    gain_ref,
    bias_ref,
    send_k,
    recv_k,
    send_ab,
    recv_a,
    recv_ab,
    send_sum,
    recv_sum,
    send_own,
    recv_own,
    send_sem,
    recv_sem,
):
    tile_rows, tile_cols, channels = z_ref.shape
    devices = row_count * col_count
    hidden = outw_ref.shape[1]
    half = col_count // 2
    width = tile_cols // CHUNKS
    pairs = tile_rows * width
    owners = row_count * half
    own = hidden // owners
    lanes = own * width
    blocks = pairs // lanes
    tokens = row_count * tile_rows
    row, col = lax.axis_index("row"), lax.axis_index("col")
    near, inner = col // half, lax.rem(col, half)
    me = row * half + inner

    def flips(index, count):
        bits = count.bit_length() - 1
        moves = [(1 << b) * (1 - 2 * lax.rem(index // (1 << b), 2)) for b in range(bits)]

        def flipped(pattern):
            total = index
            for b in range(bits):
                if pattern >> b & 1:
                    total = total + moves[b]
            return total

        return [flipped(pattern) for pattern in range(count)]

    rows, cols = flips(row, row_count), flips(col, col_count)
    row_order = sorted(range(row_count), key=lambda p: (-p.bit_count(), -p))
    across = list(range(half, col_count))
    within = list(range(half - 1, -1, -1))

    def each(action, turns):
        for turn in turns:
            for step in row_order:
                if turn or step:
                    action(rows[step], cols[turn])

    barrier = pltpu.get_barrier_semaphore()

    def greet(trow, tcol):
        pl.semaphore_signal(barrier, inc=1, device_id=(trow, tcol), device_id_type=MESH)

    each(greet, within)
    greet(row, cols[half])

    def send(source, target, at, trow, tcol):
        pltpu.make_async_remote_copy(
            src_ref=source,
            dst_ref=target,
            send_sem=send_sem.at[at],
            recv_sem=recv_sem.at[at],
            device_id=(trow, tcol),
            device_id_type=MESH,
        ).start()

    def owner(trow, tcol):
        return trow * half + lax.rem(tcol, half)

    slot = inner * row_count + row

    def start_k():
        each(
            lambda trow, tcol: send(send_k.at[owner(trow, tcol)], recv_k.at[slot], 0, trow, tcol),
            within,
        )
        recv_k[slot] = send_k[me]

    def wait_k(sem):
        slots = recv_k.at[pl.ds(0, owners - 1)]
        pltpu.make_async_copy(slots, slots, sem.at[0]).wait()

    def start_sum(chunk):
        each(
            lambda trow, tcol: send(
                send_sum.at[chunk, tcol, trow],
                recv_sum.at[chunk, near * owners + me],
                CHUNKS + chunk,
                trow,
                tcol,
            ),
            (within + across if chunk else across + within),
        )
        recv_sum[chunk, near * owners + me] = send_sum[chunk, col, row]

    def wait_sum(sem, chunk):
        slots = recv_sum.at[chunk, pl.ds(0, devices - 1)]
        pltpu.make_async_copy(slots, slots, sem.at[CHUNKS + chunk]).wait()

    def start_a(chunk):
        each(
            lambda trow, tcol: send(
                send_ab.at[chunk, owner(trow, tcol), 0],
                recv_a.at[chunk, slot],
                2 * CHUNKS + chunk,
                trow,
                tcol,
            ),
            across[::-1] if chunk else across,
        )

    def start_ab(chunk):
        each(
            lambda trow, tcol: send(
                send_ab.at[chunk, owner(trow, tcol)],
                recv_ab.at[chunk, slot],
                3 * CHUNKS + chunk,
                trow,
                tcol,
            ),
            within,
        )
        recv_ab[chunk, slot] = send_ab[chunk, me]

    def wait_ab(sem, chunk):
        slots = recv_a.at[chunk]
        pltpu.make_async_copy(slots, slots, sem.at[2 * CHUNKS + chunk]).wait()
        slots = recv_ab.at[chunk, pl.ds(0, owners - 1)]
        pltpu.make_async_copy(slots, slots, sem.at[3 * CHUNKS + chunk]).wait()

    def start_own():
        each(
            lambda trow, tcol: send(
                send_own.at[lax.rem(tcol, half), trow], recv_own.at[me], 4 * CHUNKS, trow, tcol
            ),
            within,
        )
        recv_own[me] = send_own[inner, row]

    def wait_own(sem):
        slots = recv_own.at[pl.ds(0, owners - 1)]
        pltpu.make_async_copy(slots, slots, sem.at[4 * CHUNKS]).wait()

    def spread_inputs(layer):
        in_gain_ref[layer] = columns_of(in_gain[layer : layer + 1, :], lanes)
        in_bias_ref[layer] = columns_of(in_bias[layer : layer + 1, :], lanes)

    def spread_outputs(layer):
        group = lane_groups((owners, lanes), width)
        for source, kept in ((out_gain, gain_ref), (out_bias, bias_ref)):
            wide = columns_of(source[layer : layer + 1, :], lanes)
            packed = wide[0:owners]
            for k in range(1, own):
                packed = jnp.where(group == k, wide[k * owners : (k + 1) * owners], packed)
            kept[layer] = packed

    def front(layer, current, mask_flat, target_at, sent=None):
        centred = current - jnp.mean(current, axis=0, keepdims=True)
        scale = lax.rsqrt(jnp.mean(centred * centred, axis=0, keepdims=True) + epsilon)
        gain = jnp.concatenate([in_gain_ref[layer]] * blocks, axis=1)
        bias = jnp.concatenate([in_bias_ref[layer]] * blocks, axis=1)
        normed = (centred * scale * gain + bias).astype(BF16)
        for side in range(2):
            first = 2 * side * hidden
            if layer == 0:
                weights = proj_ref[layer, :, first : first + 2 * hidden]
                projected = contract_first(weights, normed)
            else:
                weights = projt_ref[first : first + 2 * hidden]
                projected = jnp.dot(weights, normed, preferred_element_type=F32)
            panel = (sigmoid(projected[:hidden]) * projected[hidden:] * mask_flat).astype(BF16)
            for block in range(blocks):
                parts = [
                    panel[k * owners : (k + 1) * owners, block * lanes : (block + 1) * lanes]
                    for k in range(own)
                ]
                for q, part in enumerate(swap_groups(parts, width)):
                    line = block * own + q
                    tmp_ref[side, line * owners : (line + 1) * owners, :] = part.astype(F32)
            for target in range(owners):
                target_at(target)[side] = tmp_ref[
                    side, pl.ds(target, tile_rows, stride=owners), :
                ].astype(BF16)
            if sent is not None:
                sent[side]()
        return normed

    def gate(layer, chunk, normed):
        gated_ref[chunk] = sigmoid(contract_first(gate_ref[layer], normed))

    def over_channels(values):
        total = jnp.sum(values, axis=0)
        shift = lanes // 2
        while shift >= width:
            total = total + pltpu.roll(total, shift, 1)
            shift //= 2
        return total * (1.0 / hidden)

    def back(layer, chunk, returned):
        centred = returned - over_channels(returned)[None]
        scale = lax.rsqrt(over_channels(centred * centred) + epsilon)
        for d in range(owners):
            tmp_ref[chunk, d * tile_rows : (d + 1) * tile_rows, :] = (
                centred[d] * scale * gain_ref[layer, d : d + 1, :] + bias_ref[layer, d : d + 1, :]
            )
        wide_blocks = []
        for block in range(blocks):
            parts = [
                tmp_ref[chunk, pl.ds(block * own + q, owners, stride=tile_rows), :] for q in range(own)
            ]
            wide_blocks.append(jnp.concatenate(swap_groups(parts, width), axis=0).astype(BF16))
        wide = jnp.concatenate(wide_blocks, axis=1)
        if layer == 1:
            return flat_ref[chunk] + gated_flat_ref[chunk] * contract_first(wide, outw_ref[layer])
        update = jnp.dot(outwt_ref[layer], wide, preferred_element_type=F32)
        return zt_ref[chunk] + gated_ref[chunk] * update

    for at in (2, 3):
        loads[at].wait()
    spread_inputs(0)
    loads[1].wait()
    mask_float = mask_ref[...].astype(F32)
    column = lax.broadcasted_iota(jnp.int32, (tile_cols, pairs), 1) % width
    mine = (
        lax.broadcasted_iota(jnp.int32, (tile_rows, pairs), 1) // width
        == lax.broadcasted_iota(jnp.int32, (tile_rows, pairs), 0)
    ).astype(F32)
    mask_flat = []
    for chunk in range(CHUNKS):
        spread = (
            column + chunk * width == lax.broadcasted_iota(jnp.int32, (tile_cols, pairs), 0)
        ).astype(F32)
        mask_flat.append(
            jnp.sum(
                jnp.dot(mask_float, spread, preferred_element_type=F32) * mine,
                axis=0,
                keepdims=True,
            )
        )
    loads[0].wait()
    loads[4].wait()
    normed = [None] * CHUNKS
    for chunk in range(CHUNKS):
        zt_ref[chunk] = jnp.transpose(
            z_ref[:, chunk * width : (chunk + 1) * width, :].astype(F32).reshape(pairs, channels)
        )
        normed[chunk] = front(
            0,
            zt_ref[chunk],
            mask_flat[chunk],
            lambda target, chunk=chunk: send_k.at[target, chunk],
        )
    pl.semaphore_wait(barrier, owners)
    start_k()
    for at in (5, 6, 7, 8):
        loads[at].wait()
    for layer in range(1, 2):
        projt_ref[...] = jnp.transpose(proj_ref[layer])
    for layer in range(2):
        outwt_ref[layer] = jnp.transpose(outw_ref[layer])
    for chunk in range(CHUNKS):
        gate(0, chunk, normed[chunk])
    spread_inputs(1)
    for layer in range(2):
        spread_outputs(layer)
    wait_k(recv_sem)

    def panel(ref, plane, *at):
        span = (slice(plane * row_count, (plane + 1) * row_count),)
        return ref[at[:1] + span + at[1:] if ref is not recv_k else span + at].reshape(tokens, lanes)

    spans = [(chunk, plane) for chunk in range(CHUNKS) for plane in range(half)]
    lane_group = lane_groups((1, len(spans) * lanes), width) % own

    def sums(chunk):
        left = jnp.concatenate([panel(recv_k, p, c, 0) for c, p in spans], axis=1)
        right = jnp.concatenate([panel(recv_k, p, c, 1) for c, p in spans], axis=1)
        masks = [(lane_group == k).astype(F32).astype(BF16) for k in range(own)]
        for c in range(col_count):
            at = (c * CHUNKS + chunk) * width
            lines = right[at : at + width]
            stacked = jnp.concatenate([lines * masks[k] for k in range(own)], axis=0)
            product = lax.dot_general(
                left, stacked, (((1,), (1,)), ((), ())), preferred_element_type=F32
            )
            send_sum[chunk, c] = product.astype(BF16).reshape(row_count, tile_rows, lanes)
        start_sum(chunk)

    sums(0)
    for chunk in range(1, CHUNKS):
        pl.when(row >= 0)(lambda chunk=chunk: sums(chunk))

    for chunk in range(CHUNKS):
        wait_sum(recv_sem, chunk)
        returned = recv_sum[chunk, 0:owners].astype(F32) + recv_sum[
            chunk, owners : 2 * owners
        ].astype(F32)
        zt_ref[chunk] = back(0, chunk, returned)
        normed[chunk] = front(
            1,
            zt_ref[chunk],
            mask_flat[chunk],
            lambda target, chunk=chunk: send_ab.at[chunk, target],
            (
                (lambda chunk=chunk: start_a(chunk), lambda chunk=chunk: start_ab(chunk))
                if chunk < CHUNKS - 1
                else (lambda: None, lambda chunk=chunk: (start_a(chunk), start_ab(chunk)))
            ),
        )
    for chunk in range(CHUNKS):
        gated_flat_ref[chunk] = sigmoid(contract_first(normed[chunk], gate_ref[1]))
        flat_ref[chunk] = jnp.transpose(zt_ref[chunk])
    group = lane_groups((width, lanes), width)

    def pieces(left_chunk, chunk):
        right = jnp.concatenate([panel(recv_ab, p, chunk, 1) for p in range(half)], axis=1)
        for mine in range(2):
            left = jnp.concatenate(
                [
                    panel(recv_ab, p, left_chunk, 0) if mine else panel(recv_a, p, left_chunk)
                    for p in range(half)
                ],
                axis=1,
            )
            product = contract_first(left, right)
            base = (near if mine else 1 - near) * half
            for q in range(half):
                at = q * lanes
                for p in range(half):
                    piece = product[at : at + width, p * lanes : (p + 1) * lanes]
                    for k in range(1, own):
                        low = at + k * width
                        piece = jnp.where(
                            group == k,
                            product[low : low + width, p * lanes : (p + 1) * lanes],
                            piece,
                        )
                    send_own[p, (base + q) * CHUNKS + left_chunk, chunk] = piece.astype(BF16)

    for chunk in range(CHUNKS):
        wait_ab(recv_sem, chunk)
        if chunk < CHUNKS - 1:
            for other in range(chunk + 1):
                pieces(chunk, other)
                if other < chunk:
                    pieces(other, chunk)
    last = CHUNKS - 1
    for chunk in range(last):
        pieces(last, chunk)
    for other in range(CHUNKS):
        pieces(other, last)
    start_own()

    wait_own(recv_sem)
    for chunk in range(CHUNKS):
        final = back(1, chunk, recv_own[:, chunk].astype(F32))
        out_ref[:, chunk * width : (chunk + 1) * width, :] = (
            final.reshape(tile_rows, width, channels).astype(BF16)
        )
    for chunk in range(CHUNKS):
        wait_sum(send_sem, chunk)
        wait_ab(send_sem, chunk)
    wait_own(send_sem)
    wait_k(send_sem)


def fused(row_count, col_count, *args):
    tile_rows, tile_cols, channels = args[0].shape
    devices = row_count * col_count
    hidden = args[-1].shape[1]
    half = col_count // 2
    owners = row_count * half
    width = tile_cols // CHUNKS
    lanes = hidden // owners * width
    pairs = tile_rows * width
    vmem = pl.BlockSpec(memory_space=pltpu.VMEM)
    return pl.pallas_call(
        functools.partial(fused_kernel, row_count, col_count),
        out_shape=jax.ShapeDtypeStruct(args[0].shape, BF16),
        in_specs=[pl.BlockSpec(memory_space=pl.ANY)] * len(args),
        out_specs=vmem,
        scratch_shapes=[pltpu.VMEM(arg.shape, arg.dtype) for arg in args]
        + [
            pltpu.SemaphoreType.DMA((len(args),)),
            pltpu.VMEM((CHUNKS, channels, pairs), F32),
            pltpu.VMEM((2, tile_rows * owners, lanes), F32),
            pltpu.VMEM((CHUNKS, channels, pairs), F32),
            pltpu.VMEM((CHUNKS, pairs, channels), F32),
            pltpu.VMEM((CHUNKS, pairs, channels), F32),
            pltpu.VMEM(args[4].shape[:0:-1], BF16),
            pltpu.VMEM(args[8].shape[:1] + args[8].shape[:0:-1], BF16),
            pltpu.VMEM((2, channels, lanes), F32),
            pltpu.VMEM((2, channels, lanes), F32),
            pltpu.VMEM((2, owners, lanes), F32),
            pltpu.VMEM((2, owners, lanes), F32),
            pltpu.VMEM((owners, CHUNKS, 2, tile_rows, lanes), BF16),
            pltpu.VMEM((owners, CHUNKS, 2, tile_rows, lanes), BF16),
            pltpu.VMEM((CHUNKS, owners, 2, tile_rows, lanes), BF16),
            pltpu.VMEM((CHUNKS, owners, tile_rows, lanes), BF16),
            pltpu.VMEM((CHUNKS, owners, 2, tile_rows, lanes), BF16),
            pltpu.VMEM((CHUNKS, col_count, row_count, tile_rows, lanes), BF16),
            pltpu.VMEM((CHUNKS, devices, tile_rows, lanes), BF16),
            pltpu.VMEM((half, row_count, CHUNKS, tile_rows, lanes), BF16),
            pltpu.VMEM((owners, CHUNKS, tile_rows, lanes), BF16),
            pltpu.SemaphoreType.DMA((5 * CHUNKS,)),
            pltpu.SemaphoreType.DMA((5 * CHUNKS,)),
        ],
        compiler_params=pltpu.CompilerParams(
            collective_id=0, has_side_effects=True, vmem_limit_bytes=16 << 20
        ),
    )(*[pltpu.with_memory_space_constraint(arg, pltpu.HBM) for arg in args])


def solution(mesh):
    row_count, col_count = mesh.shape["row"], mesh.shape["col"]
    devices = row_count * col_count

    def step(*args):
        tile_rows, tile_cols, channels = args[0].shape
        hidden = args[-1].shape[1]
        owners = devices // 2
        own = hidden // owners
        width = tile_cols // CHUNKS
        fits = (
            hidden % devices == 0
            and col_count % 2 == 0
            and tile_cols % CHUNKS == 0
            and own * width == 128
            and tile_rows == width
            and tile_rows % 16 == 0
            and tile_rows % own == 0
            and own & (own - 1) == 0
            and row_count & (row_count - 1) == 0
            and col_count & (col_count - 1) == 0
            and row_count * tile_rows == col_count * tile_cols
        )
        return fused(row_count, col_count, *args) if fits else on_device(*args)

    return jax.shard_map(
        step,
        mesh=mesh,
        in_specs=(P("row", "col", None), P("row", "col"), P(), P(), P(), P(), P(), P(), P()),
        out_specs=P("row", "col", None),
        check_vma=False,
    )
```
